32 devices in a mesh: batch: 16 (over z, x, core), space: 2 (over y).
Axes of the slice: x: 2, y: 2, z: 4, core: 2. Of those that a mesh axis runs over, the one named last changes fastest.
Arguments:
- latents: float32 [16, 32, 64, 4], P('batch', 'space'), may hold values from -16 to 16
- noise_draw: float32 [16, 32, 64, 4], P('batch', 'space'), may hold values from -5 to 5
- timesteps: int32 [16], P('batch'), may hold values from 200 to 799
- inlet_conv: bfloat16 [36, 320], replicated, may hold values from -1 to 1
- time_first: bfloat16 [320, 1280], P(None, 'batch'), may hold values from -0.3125 to 0.3125
- time_first_bias: float32 [1280], replicated, may hold values from -4 to 4
- time_second: bfloat16 [1280, 320], P(None, 'batch'), may hold values from -0.3125 to 0.3125
- time_second_bias: float32 [320], replicated, may hold values from -4 to 4
- conv_first: bfloat16 [2880, 320], P(None, 'batch'), may hold values from -0.109375 to 0.109375
- conv_second: bfloat16 [2880, 320], P(None, 'batch'), may hold values from -0.109375 to 0.109375
- proj_inner: bfloat16 [320, 320], P(None, 'batch'), may hold values from -0.3125 to 0.3125
- query_weight: bfloat16 [320, 320], P(None, 'batch'), may hold values from -30 to 30
- key_weight: bfloat16 [320, 320], P(None, 'batch'), may hold values from -1 to 1
- value_weight: bfloat16 [320, 320], P(None, 'batch'), may hold values from -0.625 to 0.625
- attn_out: bfloat16 [320, 320], P(None, 'batch'), may hold values from -0.625 to 0.625
- proj_outer: bfloat16 [320, 320], P(None, 'batch'), may hold values from -0.3125 to 0.3125
- outlet_conv: bfloat16 [2880, 4], replicated, may hold values from -0.109375 to 0.109375
- first_gain: float32 [320], replicated, may hold values from 0.1 to 1.9
- second_gain: float32 [320], replicated, may hold values from 0.1 to 1.9
- third_gain: float32 [320], replicated, may hold values from 0.1 to 1.9
- final_gain: float32 [320], replicated, may hold values from 0.1 to 1.9
- layer_gain: float32 [320], replicated, may hold values from 0.1 to 1.9
Outputs:
- guidance: float32 [16, 32, 64, 4], P('batch', 'space')
The draws below stay inside these ranges and needn't reach their ends.
All inputs are finite; a program needn't handle non-finite values.
Results may differ from the reference program's by a relative error of at most 0.029.
Values may be sent and summed in bfloat16 or wider, within the bound.
No kernel may reach another device: no remote copies, remote signals or barrier semaphores. Data moves between devices by JAX's collectives and lax.ppermute only.
A program may use at most 128 MiB of HBM per device.

```python
import math
import jax
import jax.numpy as jnp
from jax import lax

C = 320
TEMB = 1280
HEADS = 8
HEAD_SIZE = 40
GROUPS = 32
LAT = 4
H = 32
W = 64
STEPS = 1000
VIEWS = 16


def draw_latents(key, part):
    shape = (VIEWS, H, W, LAT)
    ramp = jnp.exp(jnp.linspace(0.0, math.log(4.0), H, dtype=jnp.float32))[None, :, None, None]
    field = jax.random.truncated_normal(jax.random.fold_in(key, 7), -4.0, 4.0, shape, jnp.float32) * ramp
    return jnp.clip(field, -16.0, 16.0)


def attention_pair(key):
    shape = (C, C)
    key_part = jax.random.truncated_normal(jax.random.fold_in(key, 11), -6.0, 6.0, shape, jnp.float32) / math.sqrt(C)
    free_part = jax.random.truncated_normal(jax.random.fold_in(key, 12), -6.0, 6.0, shape, jnp.float32) / math.sqrt(C)
    query_part = 2.5 * free_part
    return (jnp.clip(query_part, -30.0, 30.0), jnp.clip(key_part, -1.0, 1.0))


def draw_query_weight(key, part):
    return attention_pair(key)[0].astype(jnp.bfloat16)


def draw_key_weight(key, part):
    return attention_pair(key)[1].astype(jnp.bfloat16)


def touch_ends(array, own_key, smallest, high):
    place = [jax.random.randint(jax.random.fold_in(own_key, axis), (), 0, length) for axis, length in enumerate(array.shape)]
    main_axis = array.shape.index(max(array.shape))
    beside = place[:main_axis] + [(place[main_axis] + 1) % array.shape[main_axis]] + place[main_axis + 1:]
    return array.at[tuple(place)].set(smallest).at[tuple(beside)].set(high)


def level_of(stream_key, dims, pieces, smallest, high):
    def one(axis_at, parts):
        heights = jax.random.uniform(jax.random.fold_in(jax.random.fold_in(stream_key, 6), axis_at), (parts,), jnp.float32, smallest / len(pieces), high / len(pieces))
        return jnp.repeat(jnp.exp(heights), dims[axis_at] // parts).reshape((-1,) + (1,) * (len(dims) - axis_at - 1))

    loudness = one(*pieces[0])
    for cut in pieces[1:]:
        loudness = loudness * one(*cut)
    return loudness


def scatter_about(key, extent, width, limit, pieces=(), kind=jnp.bfloat16):
    drawn = jax.random.normal(key, extent, jnp.float32) * width
    if len(pieces) > 0:
        drawn = level_of(key, extent, pieces, -0.22, 0.18) * drawn
    return jnp.clip(drawn, min=-limit, max=limit).astype(kind)


def setup_inputs(seed: int = 0) -> dict:
    streams_of = jax.random.split(jax.random.key(seed), 23)
    latents = draw_latents(jax.random.fold_in(streams_of[22], 71), 0)
    noise_draw = scatter_about(streams_of[1], (VIEWS, H, W, LAT), 1.0, 5.0, ((0, 16), (1, 2)), jnp.float32)
    timesteps = touch_ends(jax.random.randint(streams_of[2], (VIEWS,), 200, 800), jax.random.fold_in(streams_of[2], 1), 200, 799).astype(jnp.int32)
    inlet_conv = scatter_about(streams_of[3], (9 * LAT, C), (9 * LAT) ** -0.5, 1.0)
    time_first = scatter_about(streams_of[4], (C, TEMB), C ** -0.5, 0.3125, ((1, 16),))
    time_first_bias = scatter_about(streams_of[5], (TEMB,), 1.0, 4.0, (), jnp.float32)
    time_second = scatter_about(streams_of[6], (TEMB, C), (TEMB // 4) ** -0.5, 0.3125, ((1, 16),))
    time_second_bias = scatter_about(streams_of[7], (C,), 1.0, 4.0, (), jnp.float32)
    conv_first = scatter_about(streams_of[8], (9 * C, C), (9 * C) ** -0.5, 0.109375, ((1, 16),))
    conv_second = scatter_about(streams_of[9], (9 * C, C), (9 * C) ** -0.5, 0.109375, ((1, 16),))
    proj_inner = scatter_about(streams_of[10], (C, C), C ** -0.5, 0.3125, ((1, 16),))
    query_weight = draw_query_weight(jax.random.fold_in(streams_of[22], 71), 0)
    key_weight = draw_key_weight(jax.random.fold_in(streams_of[22], 71), 0)
    value_weight = scatter_about(streams_of[13], (C, C), (C // 4) ** -0.5, 0.625, ((1, 16),))
    attn_out = scatter_about(streams_of[14], (C, C), (C // 4) ** -0.5, 0.625, ((1, 16),))
    proj_outer = scatter_about(streams_of[15], (C, C), C ** -0.5, 0.3125, ((1, 16),))
    outlet_conv = scatter_about(streams_of[16], (9 * C, LAT), (9 * C) ** -0.5, 0.109375)
    first_gain = jnp.clip(1.0 + 0.18 * jax.random.normal(streams_of[17], (C,), jnp.float32), 0.1, 1.9)
    second_gain = jnp.clip(1.0 + 0.18 * jax.random.normal(streams_of[18], (C,), jnp.float32), 0.1, 1.9)
    third_gain = jnp.clip(1.0 + 0.18 * jax.random.normal(streams_of[19], (C,), jnp.float32), 0.1, 1.9)
    final_gain = jnp.clip(1.0 + 0.18 * jax.random.normal(streams_of[20], (C,), jnp.float32), 0.1, 1.9)
    layer_gain = jnp.clip(1.0 + 0.18 * jax.random.normal(streams_of[21], (C,), jnp.float32), 0.1, 1.9)
    return {"latents": latents, "noise_draw": noise_draw, "timesteps": timesteps, "inlet_conv": inlet_conv, "time_first": time_first, "time_first_bias": time_first_bias, "time_second": time_second, "time_second_bias": time_second_bias, "conv_first": conv_first, "conv_second": conv_second, "proj_inner": proj_inner, "query_weight": query_weight, "key_weight": key_weight, "value_weight": value_weight, "attn_out": attn_out, "proj_outer": proj_outer, "outlet_conv": outlet_conv, "first_gain": first_gain, "second_gain": second_gain, "third_gain": third_gain, "final_gain": final_gain, "layer_gain": layer_gain}


EPS_GROUP = 1e-06
EPS_BLOCK = 1e-05
EPS_LAYER = 1e-05

def plan():
    fraction = jnp.arange(STEPS, dtype=jnp.float32) / (STEPS - 1)
    beta_root = math.sqrt(0.00085) + fraction * (math.sqrt(0.012) - math.sqrt(0.00085))
    return jnp.cumprod(1.0 - beta_root * beta_root)

def lookup(timesteps):
    plan_tab = plan()
    matches = jnp.arange(STEPS, dtype=jnp.int32)[None, :] == timesteps[:, None]
    return lax.optimization_barrier(jnp.sum(jnp.where(matches, plan_tab[None, :], 0.0), axis=1))

def time_embed(timesteps, first, first_bias, second, second_bias):
    halfway = first.shape[0] // 2
    frequency = jnp.exp(-math.log(10000.0) * jnp.arange(halfway, dtype=jnp.float32) / halfway)
    angles = timesteps.astype(jnp.float32)[:, None] * frequency[None, :]
    waveform = jnp.concatenate([jnp.cos(angles), jnp.sin(angles)], axis=1).astype(jnp.bfloat16)
    inner = jax.nn.silu(jnp.dot(waveform, first, preferred_element_type=jnp.float32) + first_bias)
    hidden = jax.nn.silu(inner).astype(jnp.bfloat16)
    return jnp.dot(hidden, second, preferred_element_type=jnp.float32) + second_bias

def convolve(field, kernel):
    height, breadth, width_in = field.shape
    padded = jnp.pad(field, ((1, 1), (1, 1), (0, 0)))
    result = jnp.zeros((height, breadth, kernel.shape[1]), jnp.float32)
    for offset in range(9):
        row_off, col_off = (offset // 3, offset % 3)
        window = padded[row_off:row_off + height, col_off:col_off + breadth, :].astype(jnp.float32)
        taps = kernel[offset * width_in:(offset + 1) * width_in].astype(jnp.float32)
        result = result + jnp.einsum('hwc,cd->hwd', window, taps)
    return result

def group_norm(field, gain_vec, epsilon):
    height, breadth, chan_n = field.shape
    grouped = field.reshape(height, breadth, GROUPS, chan_n // GROUPS)
    number = height * breadth * (chan_n // GROUPS)
    means = lax.optimization_barrier(jnp.sum(grouped, axis=(0, 1, 3))) / number
    squares = lax.optimization_barrier(jnp.sum(grouped * grouped, axis=(0, 1, 3))) / number
    factor = lax.rsqrt(squares - means * means + epsilon)
    normal_f = (grouped - means[:, None]) * factor[:, None]
    return normal_f.reshape(height, breadth, chan_n) * gain_vec

def layer_norm(field, gain_vec):
    means = lax.optimization_barrier(jnp.mean(field, axis=-1, keepdims=True))
    centred = field - means
    spread = lax.optimization_barrier(jnp.mean(centred * centred, axis=-1, keepdims=True))
    return centred * lax.rsqrt(spread + EPS_LAYER) * gain_vec

def attend(queries, key_rows, value_rows):
    token_n = queries.shape[0]
    factor = 1.0 / math.sqrt(HEAD_SIZE)

    def arrange(field):
        return field.reshape(token_n, HEADS, HEAD_SIZE).transpose(1, 0, 2)

    def one_head(items):
        query_one, key_one, value_one = items
        scores = jnp.dot(query_one, key_one.T, preferred_element_type=jnp.float32) * factor
        row_max = lax.optimization_barrier(jnp.max(scores, axis=1, keepdims=True))
        weights = jnp.exp(scores - row_max)
        row_sum = lax.optimization_barrier(jnp.sum(weights, axis=1, keepdims=True))
        return jnp.dot(weights.astype(jnp.bfloat16), value_one, preferred_element_type=jnp.float32) / row_sum
    outputs = lax.map(one_head, (arrange(queries), arrange(key_rows), arrange(value_rows)))
    return outputs.transpose(1, 0, 2).reshape(token_n, HEADS * HEAD_SIZE).astype(jnp.bfloat16)

def reference(latents, noise_draw, timesteps, inlet_conv, time_first, time_first_bias, time_second, time_second_bias, conv_first, conv_second, proj_inner, query_weight, key_weight, value_weight, attn_out, proj_outer, outlet_conv, first_gain, second_gain, third_gain, final_gain, layer_gain):
    abar_all = lookup(timesteps)
    embed_all = time_embed(timesteps, time_first, time_first_bias, time_second, time_second_bias)

    def one_view(items):
        latent_one, noise_one, embed_one, abar = items
        noisy = (jnp.sqrt(abar) * latent_one + jnp.sqrt(1.0 - abar) * noise_one).astype(jnp.bfloat16)
        opening = convolve(noisy, inlet_conv).astype(jnp.bfloat16)
        active = jax.nn.silu(group_norm(opening.astype(jnp.float32), first_gain, EPS_BLOCK)).astype(jnp.bfloat16)
        middle = (convolve(active, conv_first) + embed_one).astype(jnp.bfloat16)
        active = jax.nn.silu(group_norm(middle.astype(jnp.float32), second_gain, EPS_BLOCK)).astype(jnp.bfloat16)
        block_one = (opening.astype(jnp.float32) + convolve(active, conv_second)).astype(jnp.bfloat16)
        normed = group_norm(block_one.astype(jnp.float32), third_gain, EPS_GROUP).astype(jnp.bfloat16)
        height, breadth, chan_n = normed.shape
        flattened = normed.reshape(height * breadth, chan_n)
        projected = jnp.dot(flattened, proj_inner, preferred_element_type=jnp.float32)
        tokens_in = layer_norm(projected, layer_gain).astype(jnp.bfloat16)
        queries = jnp.dot(tokens_in, query_weight, preferred_element_type=jnp.float32).astype(jnp.bfloat16)
        key_rows = jnp.dot(tokens_in, key_weight, preferred_element_type=jnp.float32).astype(jnp.bfloat16)
        value_rows = jnp.dot(tokens_in, value_weight, preferred_element_type=jnp.float32).astype(jnp.bfloat16)
        attended = attend(queries, key_rows, value_rows)
        mixture = (jnp.dot(attended, attn_out, preferred_element_type=jnp.float32) + projected).astype(jnp.bfloat16)
        outer = jnp.dot(mixture, proj_outer, preferred_element_type=jnp.float32).reshape(height, breadth, chan_n)
        block_two = (block_one.astype(jnp.float32) + outer).astype(jnp.bfloat16)
        active = jax.nn.silu(group_norm(block_two.astype(jnp.float32), final_gain, EPS_BLOCK)).astype(jnp.bfloat16)
        predicted = convolve(active, outlet_conv)
        return (1.0 - abar) * (predicted - noise_one)
    return lax.map(one_view, (latents, noise_draw, embed_all, abar_all))
```

```python
import math

import jax
import jax.numpy as jnp
from jax import lax
from jax.experimental import pallas as pl
from jax.experimental.pallas import tpu as pltpu
from jax.sharding import PartitionSpec as P

HEADS = 8
HEAD_SIZE = 40
GROUPS = 32
STEPS = 1000
EPS_GROUP = 1e-06
EPS_BLOCK = 1e-05
EPS_LAYER = 1e-05
VMEM_BYTES = 60 << 20
RING_LIMIT = 16
F32 = jnp.float32
BF16 = jnp.bfloat16


def plan():
    fraction = jnp.arange(STEPS, dtype=F32) / (STEPS - 1)
    beta_root = math.sqrt(0.00085) + fraction * (math.sqrt(0.012) - math.sqrt(0.00085))
    return jnp.cumprod(1.0 - beta_root * beta_root)


def lookup(timesteps):
    matches = jnp.arange(STEPS, dtype=jnp.int32)[None, :] == timesteps[:, None]
    return jnp.sum(jnp.where(matches, plan()[None, :], 0.0), axis=1)


def waveform_of(timesteps, halfway):
    frequency = jnp.exp(-math.log(10000.0) * jnp.arange(halfway, dtype=F32) / halfway)
    angles = timesteps.astype(F32)[:, None] * frequency[None, :]
    return jnp.concatenate([jnp.cos(angles), jnp.sin(angles)], axis=1).astype(BF16)


def batch_ring(count):
    side = count // 4
    ring = 2 * side

    def group(spot):
        spot = spot % ring
        deep, wide = (spot, 0) if spot < side else (ring - 1 - spot, 1)
        return 2 * deep + wide

    onward = []
    for spot in range(ring):
        onward.append((2 * group(spot), 2 * group(spot + 1)))
        onward.append((2 * group(spot) + 1, 2 * group(spot - 1) + 1))
    sibling = [(place, place ^ 1) for place in range(count)]
    half = ring // 2
    spot_of = [0] * (count // 2)
    for spot in range(ring):
        spot_of[group(spot)] = spot
    table = []
    for place in range(count):
        core, spot = place % 2, spot_of[place // 2]
        row = [place, place ^ 1]
        step = -1 if core == 0 else 1
        for far in range(1, half):
            mine = group(spot + step * far)
            row += [2 * mine + core, 2 * mine + (core ^ 1)]
            theirs = group(spot - step * far)
            row += [2 * theirs + (core ^ 1), 2 * theirs + core]
        far_one = group(spot + step * half)
        row += [2 * far_one + core, 2 * far_one + (core ^ 1)]
        table.append(row)
    return onward, sibling, half, table


def gather_shards(shards, beside):
    count = lax.axis_size("batch")
    if count % 4 or count > RING_LIMIT:
        whole = [[lax.all_gather(shard, "batch", axis=0, tiled=True)] for shard in shards]
        return whole, jnp.arange(count, dtype=jnp.int32), beside()
    onward, sibling, half, table = batch_ring(count)
    rows = shards[0].shape[0]
    others = [lax.ppermute(shard, "batch", sibling) for shard in shards]
    moving = [pair_up(shard, other) for shard, other in zip(shards, others)]
    gathered = [[pair] for pair in moving]
    extra = None
    for step in range(1, half):
        moving = [lax.ppermute(pair, "batch", onward) for pair in moving]
        if extra is None:
            extra = beside()
            moving, extra = lax.optimization_barrier((moving, extra))
        for pieces, pair in zip(gathered, moving):
            pieces += [pair, lax.ppermute(pair, "batch", sibling)]
    for pieces, pair in zip(gathered, moving):
        last = lax.ppermute(pair[:rows], "batch", onward)
        pieces += [last, lax.ppermute(last, "batch", sibling)]
    origin = jnp.asarray(table, dtype=jnp.int32)[lax.axis_index("batch")]
    return gathered, origin, extra


def lane_sums(value):
    total = value[:, :128]
    for start in range(128, value.shape[1], 128):
        total = total + value[:, start : start + 128]
    return total


def group_moments(sums, squares, number):
    chan_n = sums.shape[0]
    size = chan_n // GROUPS
    rows = lax.broadcasted_iota(jnp.int32, (chan_n, chan_n), 0) // size
    cols = lax.broadcasted_iota(jnp.int32, (chan_n, chan_n), 1) // size
    member = jnp.where(rows == cols, 1.0, 0.0).astype(F32)
    both = jnp.concatenate([sums, squares], axis=1)
    grouped = jnp.dot(member, both, preferred_element_type=F32, precision=lax.Precision.HIGHEST)
    mean = jnp.sum(grouped[:, :128], axis=1, keepdims=True) / number
    square = jnp.sum(grouped[:, 128:], axis=1, keepdims=True) / number
    return mean, square


def padded(rows):
    return -(-rows // 16) * 16


def assemble(origin_ref, pieces, stage, rows, out_ref):
    total, deep = out_ref.shape[0], stage.shape[0]
    rid = lax.broadcasted_iota(jnp.int32, (total, deep), 0)
    cid = lax.broadcasted_iota(jnp.int32, (total, deep), 1)
    want = jnp.full((total, deep), -1, jnp.int32)
    place = base = 0
    for ref in pieces:
        size = ref.shape[0]
        stage[base : base + size, :] = ref[...]
        if padded(size) > size:
            fill = jnp.zeros((padded(size) - size, stage.shape[1]), stage.dtype)
            stage[base + size : base + padded(size), :] = fill
        for sub in range(size // rows):
            first = base + sub * rows
            inside = (cid >= first) & (cid < first + rows)
            want = jnp.where(inside, origin_ref[place] * rows + cid - first, want)
            place += 1
        base += padded(size)
    pick = jnp.where(rid == want, 1.0, 0.0).astype(BF16)
    width = stage.shape[1]
    for start in range(0, width, 512):
        stop = min(width, start + 512)
        out_ref[:, start:stop] = jnp.dot(
            pick, stage[:, start:stop], preferred_element_type=F32
        ).astype(BF16)


def spread_taps(load, store, chan_n, token_n, breadth, chunk=16):
    def one(index, carry):
        base = pl.multiple_of(index * chunk, chunk)
        value = load(base, chunk)
        lane = lax.broadcasted_iota(jnp.int32, (chunk, token_n), 1)
        column = lane % breadth
        left = jnp.where(column == 0, 0.0, pltpu.roll(value, 1, 1))
        right = jnp.where(column == breadth - 1, 0.0, pltpu.roll(value, token_n - 1, 1))
        for col, variant in enumerate((left, value, right)):
            up = jnp.where(lane < breadth, 0.0, pltpu.roll(variant, breadth, 1))
            down = jnp.where(
                lane >= token_n - breadth, 0.0, pltpu.roll(variant, token_n - breadth, 1)
            )
            for row, shifted in enumerate((up, variant, down)):
                store((3 * row + col) * chan_n + base, chunk, shifted.astype(BF16))
        return carry

    lax.fori_loop(0, chan_n // chunk, one, 0)


def silu(value):
    return value / (1.0 + jnp.exp(-value))


def normal_taps(source_ref, taps_ref, mean_ref, factor_ref, breadth):
    chan_n, token_n = source_ref.shape

    def load(base, chunk):
        value = source_ref[pl.ds(base, chunk), :].astype(F32)
        mean = mean_ref[pl.ds(base, chunk), 0:1]
        factor = factor_ref[pl.ds(base, chunk), 0:1]
        return silu((value - mean) * factor)

    def store(base, chunk, value):
        taps_ref[pl.ds(pl.multiple_of(base, chunk), chunk), :] = value

    spread_taps(load, store, chan_n, token_n, breadth)


def set_moments(sums, squares, number, gain, epsilon, mean_ref, factor_ref):
    mean, square = group_moments(sums, squares, number)
    factor = lax.rsqrt(square - mean * mean + epsilon) * gain
    mean_ref[...] = jnp.broadcast_to(mean, mean_ref.shape)
    factor_ref[...] = jnp.broadcast_to(factor, factor_ref.shape)


def pair_kernel(one_ref, two_ref, out_ref):
    rows = one_ref.shape[0]
    out_ref[:rows] = one_ref[...]
    out_ref[rows:] = two_ref[...]


def pair_up(one, two):
    whole = jax.ShapeDtypeStruct((2 * one.shape[0], one.shape[1]), one.dtype)
    return kernel_call(pair_kernel, whole, [])(one, two)


def pack_kernel(conv_first, time_first, time_second, conv_second, *rest):
    squares, (one_ref, two_ref) = rest[:-2], rest[-2:]
    rows, conv_width = conv_first.shape
    chan_n = time_first.shape[1]
    one_ref[:, :conv_width] = conv_first[...]
    for index in range(time_first.shape[0] // rows):
        base = conv_width + index * chan_n
        one_ref[:, base : base + chan_n] = time_first[index * rows : (index + 1) * rows]
    one_ref[:, conv_width + time_second.shape[1] :] = time_second[...]
    two_ref[:, :conv_width] = conv_second[...]
    for index, square in enumerate(squares):
        base = conv_width + index * chan_n
        two_ref[:, base : base + chan_n] = square[...]


def opening_kernel(breadth, noisy_ref, kernel_ref, start_ref, sums_ref, squares_ref, flat, taps):
    height, lat_n, _ = noisy_ref.shape
    token_n = height * breadth
    flat[...] = jnp.zeros(flat.shape, F32)
    for row in range(height):
        flat[0:lat_n, row * breadth : (row + 1) * breadth] = noisy_ref[row].astype(F32)
    taps[...] = jnp.zeros(taps.shape, F32)
    value = flat[...]
    lane = lax.broadcasted_iota(jnp.int32, value.shape, 1)
    column = lane % breadth
    for offset in range(9):
        row_off, col_off = offset // 3 - 1, offset % 3 - 1
        shift = -(row_off * breadth + col_off) % token_n
        moved = pltpu.roll(value, shift, 1) if shift else value
        good = (column + col_off >= 0) & (column + col_off < breadth)
        good = good & (lane + row_off * breadth >= 0) & (lane + row_off * breadth < token_n)
        moved = jnp.where(good, moved, 0.0)
        taps[offset * lat_n : (offset + 1) * lat_n, :] = moved[0:lat_n]
    block_n = min(512, token_n)
    for start in range(0, token_n, block_n):
        part = jnp.dot(
            kernel_ref[...],
            taps[:, start : start + block_n].astype(BF16),
            preferred_element_type=F32,
        ).astype(BF16)
        start_ref[:, start : start + block_n] = part
        wide = part.astype(F32)
        if start == 0:
            sums_ref[...] = lane_sums(wide)
            squares_ref[...] = lane_sums(wide * wide)
        else:
            sums_ref[...] += lane_sums(wide)
            squares_ref[...] += lane_sums(wide * wide)


def first_kernel(
    counts,
    rows,
    breadth,
    origin_ref,
    start_ref,
    sums_ref,
    squares_ref,
    gains_ref,
    wave_ref,
    bias_ref,
    *rest,
):
    pieces = rest[:counts]
    middle_ref, sums_out, squares_out = rest[counts : counts + 3]
    stage, weights, taps, mean, factor, hidden = rest[counts + 3 :]
    chan_n, token_n = start_ref.shape
    number = token_n * (chan_n // GROUPS)
    assemble(origin_ref, pieces, stage, rows, weights)
    conv_width = 9 * chan_n
    temb_n = hidden.shape[0]
    many = temb_n // chan_n
    for index in range(many):
        first = weights[:, conv_width + index * chan_n : conv_width + (index + 1) * chan_n]
        inner = jnp.dot(first, wave_ref[...], preferred_element_type=F32)
        for place in range(chan_n // rows):
            base = place * many * rows + index * rows
            hidden[base : base + rows, :] = inner[place * rows : (place + 1) * rows]
    second = weights[:, conv_width + temb_n : conv_width + 2 * temb_n]
    lifted = silu(silu(hidden[...] + bias_ref[...].T[:, 0:1])).astype(BF16)
    embedded = jnp.dot(second, lifted, preferred_element_type=F32)
    embedded = embedded[:, 0:1] + gains_ref[:, 5:6]
    set_moments(
        sums_ref[...], squares_ref[...], number, gains_ref[:, 0:1], EPS_BLOCK, mean, factor
    )
    normal_taps(start_ref, taps, mean, factor, breadth)
    block_n = min(512, token_n)
    for start in range(0, token_n, block_n):
        part = jnp.dot(
            weights[:, :conv_width], taps[:, start : start + block_n], preferred_element_type=F32
        )
        part = (part + embedded).astype(BF16)
        middle_ref[:, start : start + block_n] = part
        wide = part.astype(F32)
        if start == 0:
            sums_out[...] = lane_sums(wide)
            squares_out[...] = lane_sums(wide * wide)
        else:
            sums_out[...] += lane_sums(wide)
            squares_out[...] += lane_sums(wide * wide)


def second_kernel(
    counts,
    rows,
    breadth,
    origin_ref,
    space_ref,
    middle_ref,
    sums_ref,
    squares_ref,
    start_ref,
    gains_ref,
    *rest,
):
    pieces = rest[:counts]
    block_out, projected_out, query_out, key_out, value_out, outer_out = rest[counts : counts + 6]
    stage, weights, taps, mean, factor, sums, squares, block, tokens = rest[counts + 6 :]
    chan_n, token_n = middle_ref.shape
    query_n = block_out.shape[1]
    number = token_n * (chan_n // GROUPS)
    assemble(origin_ref, pieces, stage, rows, weights)
    conv_width = 9 * chan_n

    def small(index):
        base = conv_width + index * chan_n
        return weights[:, base : base + chan_n]

    set_moments(
        sums_ref[...], squares_ref[...], number, gains_ref[:, 1:2], EPS_BLOCK, mean, factor
    )
    normal_taps(middle_ref, taps, mean, factor, breadth)
    block_n = min(512, token_n)
    for start in range(0, token_n, block_n):
        part = jnp.dot(
            weights[:, :conv_width], taps[:, start : start + block_n], preferred_element_type=F32
        )
        part = (part + start_ref[:, start : start + block_n].astype(F32)).astype(BF16)
        block[:, start : start + block_n] = part
        wide = part.astype(F32)
        if start == 0:
            sums[...] = lane_sums(wide)
            squares[...] = lane_sums(wide * wide)
        else:
            sums[...] += lane_sums(wide)
            squares[...] += lane_sums(wide * wide)
    set_moments(sums[...], squares[...], number, gains_ref[:, 2:3], EPS_GROUP, mean, factor)
    own = pl.multiple_of(space_ref[0] * query_n, 128)

    def project(source):
        normed = ((source.astype(F32) - mean[:, 0:1]) * factor[:, 0:1]).astype(BF16)
        return jnp.dot(small(0), normed, preferred_element_type=F32)

    for start in range(0, token_n, block_n):
        projected = project(block[:, start : start + block_n])
        average = jnp.mean(projected, axis=0, keepdims=True)
        centred = projected - average
        spread = jnp.mean(centred * centred, axis=0, keepdims=True)
        scaled = centred * lax.rsqrt(spread + EPS_LAYER) * gains_ref[:, 4:5]
        token = scaled.astype(BF16)
        tokens[:, start : start + block_n] = token
        value = jnp.dot(small(3), token, preferred_element_type=F32)
        ones = jnp.ones((8, block_n), F32)
        for head in range(HEADS):
            piece = value[head * HEAD_SIZE : (head + 1) * HEAD_SIZE]
            value_out[head, :, start : start + block_n] = jnp.concatenate(
                [piece, ones], axis=0
            ).astype(BF16)
        upright = scaled.T.astype(BF16)
        half = HEADS // 2 * HEAD_SIZE
        for part in range(2):
            matrix = weights[
                part * half : (part + 1) * half,
                conv_width + 2 * chan_n : conv_width + 3 * chan_n,
            ]
            key_out[part, start : start + block_n, :] = lax.dot_general(
                upright, matrix, (((1,), (1,)), ((), ())), preferred_element_type=F32
            ).astype(BF16)
    block_out[...] = block[:, pl.ds(own, query_n)]
    projected_out[...] = project(block[:, pl.ds(own, query_n)])
    query = jnp.dot(small(1), tokens[:, pl.ds(own, query_n)], preferred_element_type=F32)
    query = query * (math.log2(math.e) / math.sqrt(HEAD_SIZE))
    per_half = HEADS // 2
    for head in range(HEADS):
        spot = head % per_half
        piece = query[head * HEAD_SIZE : (head + 1) * HEAD_SIZE]
        parts = []
        if spot:
            parts.append(jnp.zeros((spot * HEAD_SIZE, query_n), F32))
        parts.append(piece)
        if spot < per_half - 1:
            parts.append(jnp.zeros(((per_half - 1 - spot) * HEAD_SIZE, query_n), F32))
        query_out[head] = jnp.concatenate(parts, axis=0).astype(BF16)
    outer_out[0] = small(4)
    outer_out[1] = small(5)


def exact_parts(value):
    high = value.astype(BF16)
    rest = value - high.astype(F32)
    middle = rest.astype(BF16)
    return [high, middle, (rest - middle.astype(F32)).astype(BF16)]


def attention_kernel(
    breadth,
    space_ref,
    query_ref,
    key_ref,
    value_ref,
    projected_ref,
    block_ref,
    outer_ref,
    block_two_ref,
    sums_ref,
    squares_ref,
    packed_ref,
    scores,
    weights,
    attended,
):
    heads, _, query_n = query_ref.shape
    token_n = key_ref.shape[1]
    width = scores.shape[1]
    per_half = heads // 2
    key_n = min(512, token_n)

    for head in range(heads):

        def one(step, carry):
            base = pl.multiple_of(step * width, 128)
            query = query_ref[head, :, pl.ds(base, width)]
            top = jnp.full((1, width), -jnp.inf, F32)
            for start in range(0, token_n, key_n):
                part = jnp.dot(
                    key_ref[head // per_half, start : start + key_n, :],
                    query,
                    preferred_element_type=F32,
                )
                scores[start : start + key_n, :] = part
                top = jnp.maximum(top, jnp.max(part, axis=0, keepdims=True))
            for start in range(0, token_n, key_n):
                weights[start : start + key_n, :] = jnp.exp2(
                    scores[start : start + key_n, :] - top
                ).astype(BF16)
            mixed = jnp.dot(value_ref[head], weights[...], preferred_element_type=F32)
            result = mixed[:HEAD_SIZE] / mixed[HEAD_SIZE : HEAD_SIZE + 1]
            attended[head * HEAD_SIZE : (head + 1) * HEAD_SIZE, pl.ds(base, width)] = result
            return carry

        lax.fori_loop(0, query_n // width, one, 0)
    mixture = jnp.dot(outer_ref[0], attended[...].astype(BF16), preferred_element_type=F32)
    mixture = (mixture + projected_ref[...]).astype(BF16)
    outer = jnp.dot(outer_ref[1], mixture, preferred_element_type=F32)
    block_two = (block_ref[...].astype(F32) + outer).astype(BF16)
    block_two_ref[...] = block_two
    wide = block_two.astype(F32)
    sums = lane_sums(wide)
    squares = lane_sums(wide * wide)
    sums_ref[...] = sums
    squares_ref[...] = squares
    edge = jnp.where(space_ref[0] == 0, wide[:, query_n - breadth :], wide[:, :breadth])
    columns = [edge.astype(BF16)]
    columns += exact_parts(jnp.sum(sums, axis=1, keepdims=True))
    columns += exact_parts(jnp.sum(squares, axis=1, keepdims=True))
    lane = lax.broadcasted_iota(jnp.int32, packed_ref.shape, 1)
    packed = jnp.zeros(packed_ref.shape, F32)
    for index, part in enumerate(columns[1:]):
        packed = jnp.where(lane == breadth + index, part.astype(F32), packed)
    packed_ref[...] = packed.astype(BF16)
    packed_ref[:, :breadth] = columns[0]


def closing_kernel(
    breadth,
    number,
    space_n,
    space_ref,
    weight_ref,
    block_ref,
    above_ref,
    below_ref,
    sums_ref,
    squares_ref,
    gains_ref,
    kernel_ref,
    noise_ref,
    out_ref,
    active,
):
    chan_n, token_n = block_ref.shape
    lat_n = noise_ref.shape[1]
    sums, squares = sums_ref[...], squares_ref[...]
    if space_n == 2:
        lane = lax.broadcasted_iota(jnp.int32, sums.shape, 1)
        peer = above_ref[...].astype(F32)
        sums = sums + jnp.where((lane >= breadth) & (lane < breadth + 3), peer, 0.0)
        squares = squares + jnp.where((lane >= breadth + 3) & (lane < breadth + 6), peer, 0.0)
    mean, square = group_moments(sums, squares, number)
    factor = lax.rsqrt(square - mean * mean + EPS_BLOCK) * gains_ref[:, 3:4]

    def act(value):
        return silu((value.astype(F32) - mean) * factor)

    first = space_ref[0] == 0
    last = space_ref[0] == space_n - 1
    margin = 2 * breadth
    top = jnp.where(first, 0.0, act(above_ref[:, :breadth]))
    end = jnp.where(last, 0.0, act(below_ref[:, :breadth]))
    blank = jnp.zeros((chan_n, breadth), F32)
    active[:, :margin] = jnp.concatenate([blank, top], axis=1).astype(BF16)
    active[:, margin : margin + token_n] = act(block_ref[...]).astype(BF16)
    active[:, margin + token_n :] = jnp.concatenate([end, blank], axis=1).astype(BF16)
    taps = jnp.dot(kernel_ref[...], active[...], preferred_element_type=F32)
    total_n = token_n + 2 * margin
    lane = lax.broadcasted_iota(jnp.int32, (8, token_n), 1)
    column = lane % breadth
    result = jnp.zeros((8, token_n), F32)
    for offset in range(9):
        row_off, col_off = offset // 3 - 1, offset % 3 - 1
        piece = taps[offset * 8 : (offset + 1) * 8]
        shift = -(row_off * breadth + col_off) % total_n
        moved = pltpu.roll(piece, shift, 1) if shift else piece
        moved = moved[:, margin : margin + token_n]
        good = (column + col_off >= 0) & (column + col_off < breadth)
        result = result + jnp.where(good, moved, 0.0)
    weight = weight_ref[0]
    for row in range(token_n // breadth):
        part = result[0:lat_n, row * breadth : (row + 1) * breadth]
        out_ref[row] = weight * (part - noise_ref[row])


def kernel_call(body, out_shape, scratch, scalars=0):
    smem = pl.BlockSpec(memory_space=pltpu.SMEM)
    vmem = pl.BlockSpec(memory_space=pltpu.VMEM)

    def call(*args):
        return pl.pallas_call(
            body,
            out_shape=out_shape,
            in_specs=[smem] * scalars + [vmem] * (len(args) - scalars),
            scratch_shapes=scratch,
            compiler_params=pltpu.CompilerParams(vmem_limit_bytes=VMEM_BYTES),
        )(*args)

    return call


def body(
    latents,
    noise_draw,
    timesteps,
    inlet_conv,
    time_first,
    time_first_bias,
    time_second,
    time_second_bias,
    conv_first,
    conv_second,
    proj_inner,
    query_weight,
    key_weight,
    value_weight,
    attn_out,
    proj_outer,
    outlet_conv,
    first_gain,
    second_gain,
    third_gain,
    final_gain,
    layer_gain,
):
    shape = jax.ShapeDtypeStruct
    view_n, height, breadth, lat_n = latents.shape
    assert view_n == 1
    rows = conv_first.shape[1]
    chan_n = inlet_conv.shape[1]
    temb_n = time_first_bias.shape[0]
    many = temb_n // chan_n
    space_n = lax.axis_size("space")
    place = lax.axis_index("space")
    token_n = height * space_n * breadth
    query_n = height * breadth

    squares = (proj_inner, query_weight, key_weight, value_weight, attn_out, proj_outer)
    shards = (conv_first, time_first, time_second, conv_second) + squares
    conv_width = conv_first.shape[0]
    width_one = conv_width + 2 * temb_n
    width_two = conv_width + len(squares) * chan_n
    batch_one, batch_two = kernel_call(
        pack_kernel,
        [shape((rows, width_one), BF16), shape((rows, width_two), BF16)],
        [],
    )(*(shard.T for shard in shards))

    moments = [shape((chan_n, 128), F32)] * 2
    taps_n = 9 * lat_n
    taps_pad = -(-taps_n // 16) * 16
    alpha_bar = lookup(timesteps)

    def early():
        alpha_here = alpha_bar[:, None, None, None]
        noisy = jnp.sqrt(alpha_here) * latents + jnp.sqrt(1.0 - alpha_here) * noise_draw
        noisy = noisy.astype(BF16)[0].transpose(0, 2, 1)
        noisy = lax.all_gather(noisy, "space", axis=0, tiled=True)
        inlet = jnp.pad(inlet_conv.T, ((0, 0), (0, taps_pad - taps_n)))
        opened = kernel_call(
            lambda *refs: opening_kernel(breadth, *refs),
            [shape((chan_n, token_n), BF16)] + moments,
            [pltpu.VMEM((8, token_n), F32), pltpu.VMEM((taps_pad, token_n), F32)],
        )(noisy, inlet)
        wave = waveform_of(timesteps, chan_n // 2)
        wave = jnp.broadcast_to(wave.reshape(chan_n, 1), (chan_n, 128))
        gains = (first_gain, second_gain, third_gain, final_gain, layer_gain, time_second_bias)
        gains = jnp.stack(gains, axis=1)
        outlet = outlet_conv.T.reshape(lat_n, 9, chan_n).transpose(1, 0, 2)
        outlet = jnp.pad(outlet, ((0, 0), (0, 8 - lat_n), (0, 0))).reshape(72, chan_n)
        bias = jnp.broadcast_to(time_first_bias[None], (8, temb_n))
        return list(opened) + [wave, gains, outlet, bias]

    (pieces_one, pieces_two), origin, extra = gather_shards((batch_one, batch_two), early)
    start, sums, squares, wave, gains, outlet, bias = extra
    space_id = place.reshape(1).astype(jnp.int32)

    count_one = len(pieces_one)
    deep = sum(padded(piece.shape[0]) for piece in pieces_one)
    args = (origin, start, sums, squares, gains, wave, bias, *pieces_one)
    middle, sums, squares = kernel_call(
        lambda *refs: first_kernel(count_one, rows, breadth, *refs),
        [shape((chan_n, token_n), BF16)] + moments,
        [
            pltpu.VMEM((deep, width_one), BF16),
            pltpu.VMEM((chan_n, width_one), BF16),
            pltpu.VMEM((9 * chan_n, token_n), BF16),
            pltpu.VMEM((chan_n, 128), F32),
            pltpu.VMEM((chan_n, 128), F32),
            pltpu.VMEM((temb_n, 128), F32),
        ],
        1,
    )(*args)

    count_two = len(pieces_two)
    half = HEADS // 2 * HEAD_SIZE
    args = (origin, space_id, middle, sums, squares, start, gains, *pieces_two)
    block, projected, query, key, value, outer = kernel_call(
        lambda *refs: second_kernel(count_two, rows, breadth, *refs),
        [
            shape((chan_n, query_n), BF16),
            shape((chan_n, query_n), F32),
            shape((HEADS, half, query_n), BF16),
            shape((2, token_n, half), BF16),
            shape((HEADS, HEAD_SIZE + 8, token_n), BF16),
            shape((2, chan_n, chan_n), BF16),
        ],
        [
            pltpu.VMEM((deep, width_two), BF16),
            pltpu.VMEM((chan_n, width_two), BF16),
            pltpu.VMEM((9 * chan_n, token_n), BF16),
            pltpu.VMEM((chan_n, 128), F32),
            pltpu.VMEM((chan_n, 128), F32),
            pltpu.VMEM((chan_n, 128), F32),
            pltpu.VMEM((chan_n, 128), F32),
            pltpu.VMEM((chan_n, token_n), BF16),
            pltpu.VMEM((chan_n, token_n), BF16),
        ],
        2,
    )(*args)

    block_w = min(256, query_n)
    block_two, sums, squares, packed = kernel_call(
        lambda *refs: attention_kernel(breadth, *refs),
        [shape((chan_n, query_n), BF16)] + moments + [shape((chan_n, 128), BF16)],
        [
            pltpu.VMEM((token_n, block_w), F32),
            pltpu.VMEM((token_n, block_w), BF16),
            pltpu.VMEM((chan_n, query_n), F32),
        ],
        1,
    )(space_id, query, key, value, projected, block, outer)

    if space_n == 2:
        above = below = lax.ppermute(packed, "space", [(0, 1), (1, 0)])
    else:
        sums, squares = lax.psum((sums, squares), "space")
        ahead = [(i, i + 1) for i in range(space_n - 1)]
        above = lax.ppermute(block_two[:, query_n - breadth :], "space", ahead)
        below = lax.ppermute(block_two[:, :breadth], "space", [(j, i) for i, j in ahead])
    number = token_n * (chan_n // GROUPS)
    args = (
        space_id,
        1.0 - alpha_bar,
        block_two,
        above,
        below,
        sums,
        squares,
        gains,
        outlet,
        noise_draw[0].transpose(0, 2, 1),
    )
    out = kernel_call(
        lambda *refs: closing_kernel(breadth, number, space_n, *refs),
        shape((height, lat_n, breadth), F32),
        [pltpu.VMEM((chan_n, query_n + 4 * breadth), BF16)],
        2,
    )(*args)
    return out.transpose(0, 2, 1)[None]


def solution(mesh):
    split = P(None, "batch")
    view = P("batch", "space", None, None)
    in_specs = (view, view, P("batch"), P(), split, P(), split, P())
    in_specs = in_specs + (split,) * 8 + (P(),) * 6
    return jax.shard_map(body, mesh=mesh, in_specs=in_specs, out_specs=view, check_vma=False)
```

```python
import math

import jax
import jax.numpy as jnp
from jax import lax
from jax.experimental import pallas as pl
from jax.experimental.pallas import tpu as pltpu
from jax.sharding import PartitionSpec as P

HEADS = 8
HEAD_SIZE = 40
GROUPS = 32
STEPS = 1000
EPS_GROUP = 1e-06
EPS_BLOCK = 1e-05
EPS_LAYER = 1e-05
VMEM_BYTES = 60 << 20
RING_LIMIT = 16
F32 = jnp.float32
BF16 = jnp.bfloat16


def plan():
    fraction = jnp.arange(STEPS, dtype=F32) / (STEPS - 1)
    beta_root = math.sqrt(0.00085) + fraction * (math.sqrt(0.012) - math.sqrt(0.00085))
    return jnp.cumprod(1.0 - beta_root * beta_root)


def lookup(timesteps):
    matches = jnp.arange(STEPS, dtype=jnp.int32)[None, :] == timesteps[:, None]
    return jnp.sum(jnp.where(matches, plan()[None, :], 0.0), axis=1)


def waveform_of(timesteps, halfway):
    frequency = jnp.exp(-math.log(10000.0) * jnp.arange(halfway, dtype=F32) / halfway)
    angles = timesteps.astype(F32)[:, None] * frequency[None, :]
    return jnp.concatenate([jnp.cos(angles), jnp.sin(angles)], axis=1).astype(BF16)


def batch_ring(count):
    side = count // 4
    ring = 2 * side

    def group(spot):
        spot = spot % ring
        deep, wide = (spot, 0) if spot < side else (ring - 1 - spot, 1)
        return 2 * deep + wide

    onward = []
    for spot in range(ring):
        onward.append((2 * group(spot), 2 * group(spot + 1)))
        onward.append((2 * group(spot) + 1, 2 * group(spot - 1) + 1))
    sibling = [(place, place ^ 1) for place in range(count)]
    half = ring // 2
    spot_of = [0] * (count // 2)
    for spot in range(ring):
        spot_of[group(spot)] = spot
    table = []
    for place in range(count):
        core, spot = place % 2, spot_of[place // 2]
        row = [place, place ^ 1]
        step = -1 if core == 0 else 1
        for far in range(1, half):
            mine = group(spot + step * far)
            row += [2 * mine + core, 2 * mine + (core ^ 1)]
            theirs = group(spot - step * far)
            row += [2 * theirs + (core ^ 1), 2 * theirs + core]
        far_one = group(spot + step * half)
        row += [2 * far_one + core, 2 * far_one + (core ^ 1)]
        table.append(row)
    return onward, sibling, half, table


def gather_shards(shards, beside):
    count = lax.axis_size("batch")
    if count % 4 or count > RING_LIMIT:
        whole = [[lax.all_gather(shard, "batch", axis=0, tiled=True)] for shard in shards]
        return whole, jnp.arange(count, dtype=jnp.int32), beside()
    onward, sibling, half, table = batch_ring(count)
    rows = shards[0].shape[0]
    others = [lax.ppermute(shard, "batch", sibling) for shard in shards]
    moving = [pair_up(shard, other) for shard, other in zip(shards, others)]
    gathered = [[pair] for pair in moving]
    table = jnp.asarray(table, dtype=jnp.int32)
    extra = None
    for step in range(1, half):
        moving = [lax.ppermute(pair, "batch", onward) for pair in moving]
        if extra is None:
            origin = table[lax.axis_index("batch")]
            moving, origin, extra = lax.optimization_barrier((moving, origin, beside()))
        for pieces, pair in zip(gathered, moving):
            pieces += [pair, lax.ppermute(pair, "batch", sibling)]
    for pieces, pair in zip(gathered, moving):
        last = lax.ppermute(pair[:rows], "batch", onward)
        pieces += [last, lax.ppermute(last, "batch", sibling)]
    return gathered, origin, extra


def lane_sums(value):
    total = value[:, :128]
    for start in range(128, value.shape[1], 128):
        total = total + value[:, start : start + 128]
    return total


def group_moments(sums, squares, number):
    chan_n = sums.shape[0]
    size = chan_n // GROUPS
    rows = lax.broadcasted_iota(jnp.int32, (chan_n, chan_n), 0) // size
    cols = lax.broadcasted_iota(jnp.int32, (chan_n, chan_n), 1) // size
    member = jnp.where(rows == cols, 1.0, 0.0).astype(F32)
    both = jnp.concatenate([sums, squares], axis=1)
    grouped = jnp.dot(member, both, preferred_element_type=F32, precision=lax.Precision.HIGHEST)
    mean = jnp.sum(grouped[:, :128], axis=1, keepdims=True) / number
    square = jnp.sum(grouped[:, 128:], axis=1, keepdims=True) / number
    return mean, square


def padded(rows):
    return -(-rows // 16) * 16


def assemble(origin_ref, pieces, stage, rows, out_ref):
    total, deep = out_ref.shape[0], stage.shape[0]
    rid = lax.broadcasted_iota(jnp.int32, (total, deep), 0)
    cid = lax.broadcasted_iota(jnp.int32, (1, deep), 1)
    want = jnp.full((1, deep), -1, jnp.int32)
    place = base = 0
    for ref in pieces:
        size = ref.shape[0]
        stage[base : base + size, :] = ref[...]
        if padded(size) > size:
            fill = jnp.zeros((padded(size) - size, stage.shape[1]), stage.dtype)
            stage[base + size : base + padded(size), :] = fill
        for sub in range(size // rows):
            first = base + sub * rows
            inside = (cid >= first) & (cid < first + rows)
            want = jnp.where(inside, origin_ref[place] * rows + cid - first, want)
            place += 1
        base += padded(size)
    pick = jnp.where(rid == want, 1.0, 0.0).astype(BF16)
    width = stage.shape[1]
    for start in range(0, width, 512):
        stop = min(width, start + 512)
        out_ref[:, start:stop] = jnp.dot(
            pick, stage[:, start:stop], preferred_element_type=F32
        ).astype(BF16)


def spread_taps(load, level_ref, offset_ref, breadth, chunk=16):
    chan_n, token_n = level_ref.shape[0] // 3, level_ref.shape[1]

    def one(index, carry):
        base = pl.multiple_of(index * chunk, chunk)
        value = load(base, chunk)
        column = lax.broadcasted_iota(jnp.int32, (chunk, token_n), 1) % breadth
        left = jnp.where(column == 0, 0.0, pltpu.roll(value, 1, 1))
        right = jnp.where(column == breadth - 1, 0.0, pltpu.roll(value, token_n - 1, 1))
        margin = lax.broadcasted_iota(jnp.int32, (chunk, 2 * breadth), 1) < breadth
        for col, variant in enumerate((left, value, right)):
            place = pl.ds(pl.multiple_of(col * chan_n + base, chunk), chunk)
            level_ref[place, :] = variant.astype(BF16)
            later = pltpu.roll(variant, breadth, 1)
            head = later[:, : 2 * breadth]
            offset_ref[place, : 2 * breadth] = jnp.where(margin, 0.0, head).astype(BF16)
            offset_ref[place, 2 * breadth : token_n] = later[:, 2 * breadth :].astype(BF16)
            offset_ref[place, token_n:] = jnp.where(margin, head, 0.0).astype(BF16)
        return carry

    lax.fori_loop(0, chan_n // chunk, one, 0)


def convolve(weights, level_ref, offset_ref, breadth, start, block_n):
    deep = level_ref.shape[0]
    total = None
    for row in range(3):
        source = level_ref if row == 1 else offset_ref
        first = start + (2 * breadth if row == 2 else 0)
        part = jnp.dot(
            weights[:, row * deep : (row + 1) * deep],
            source[:, first : first + block_n],
            preferred_element_type=F32,
        )
        total = part if total is None else total + part
    return total


def silu(value):
    return value / (1.0 + jnp.exp(-value))


def normal_taps(source_ref, level_ref, offset_ref, mean_ref, factor_ref, breadth):
    def load(base, chunk):
        value = source_ref[pl.ds(base, chunk), :].astype(F32)
        mean = mean_ref[pl.ds(base, chunk), 0:1]
        factor = factor_ref[pl.ds(base, chunk), 0:1]
        return silu((value - mean) * factor)

    spread_taps(load, level_ref, offset_ref, breadth)


def set_moments(sums, squares, number, gain, epsilon, mean_ref, factor_ref):
    mean, square = group_moments(sums, squares, number)
    factor = lax.rsqrt(square - mean * mean + epsilon) * gain
    mean_ref[...] = jnp.broadcast_to(mean, mean_ref.shape)
    factor_ref[...] = jnp.broadcast_to(factor, factor_ref.shape)


def pair_kernel(one_ref, two_ref, out_ref):
    rows = one_ref.shape[0]
    out_ref[:rows] = one_ref[...]
    out_ref[rows:] = two_ref[...]


def pair_up(one, two):
    whole = jax.ShapeDtypeStruct((2 * one.shape[0], one.shape[1]), one.dtype)
    return kernel_call(pair_kernel, whole, [])(one, two)


def pack_kernel(conv_first, time_first, time_second, conv_second, *rest):
    squares, (one_ref, two_ref) = rest[:-2], rest[-2:]
    rows, conv_width = conv_first.shape
    chan_n = time_first.shape[1]
    one_ref[:, :conv_width] = conv_first[...]
    for index in range(time_first.shape[0] // rows):
        base = conv_width + index * chan_n
        one_ref[:, base : base + chan_n] = time_first[index * rows : (index + 1) * rows]
    one_ref[:, conv_width + time_second.shape[1] :] = time_second[...]
    two_ref[:, :conv_width] = conv_second[...]
    for index, square in enumerate(squares):
        base = conv_width + index * chan_n
        two_ref[:, base : base + chan_n] = square[...]


def opening_kernel(breadth, noisy_ref, kernel_ref, start_ref, sums_ref, squares_ref, flat, taps):
    height, lat_n, _ = noisy_ref.shape
    token_n = height * breadth
    flat[...] = jnp.zeros(flat.shape, F32)
    for row in range(height):
        flat[0:lat_n, row * breadth : (row + 1) * breadth] = noisy_ref[row].astype(F32)
    taps[...] = jnp.zeros(taps.shape, F32)
    value = flat[...]
    lane = lax.broadcasted_iota(jnp.int32, value.shape, 1)
    column = lane % breadth
    for offset in range(9):
        row_off, col_off = offset // 3 - 1, offset % 3 - 1
        shift = -(row_off * breadth + col_off) % token_n
        moved = pltpu.roll(value, shift, 1) if shift else value
        good = (column + col_off >= 0) & (column + col_off < breadth)
        good = good & (lane + row_off * breadth >= 0) & (lane + row_off * breadth < token_n)
        moved = jnp.where(good, moved, 0.0)
        taps[offset * lat_n : (offset + 1) * lat_n, :] = moved[0:lat_n]
    block_n = min(512, token_n)
    for start in range(0, token_n, block_n):
        part = jnp.dot(
            kernel_ref[...],
            taps[:, start : start + block_n].astype(BF16),
            preferred_element_type=F32,
        ).astype(BF16)
        start_ref[:, start : start + block_n] = part
        wide = part.astype(F32)
        if start == 0:
            sums_ref[...] = lane_sums(wide)
            squares_ref[...] = lane_sums(wide * wide)
        else:
            sums_ref[...] += lane_sums(wide)
            squares_ref[...] += lane_sums(wide * wide)


def first_kernel(
    counts,
    rows,
    breadth,
    origin_ref,
    start_ref,
    sums_ref,
    squares_ref,
    gains_ref,
    wave_ref,
    bias_ref,
    *rest,
):
    pieces = rest[:counts]
    middle_ref, sums_out, squares_out = rest[counts : counts + 3]
    stage, weights, level, offset, mean, factor, hidden = rest[counts + 3 :]
    chan_n, token_n = start_ref.shape
    number = token_n * (chan_n // GROUPS)
    assemble(origin_ref, pieces, stage, rows, weights)
    conv_width = 9 * chan_n
    temb_n = hidden.shape[0]
    many = temb_n // chan_n
    for index in range(many):
        first = weights[:, conv_width + index * chan_n : conv_width + (index + 1) * chan_n]
        inner = jnp.dot(first, wave_ref[...], preferred_element_type=F32)
        for place in range(chan_n // rows):
            base = place * many * rows + index * rows
            hidden[base : base + rows, :] = inner[place * rows : (place + 1) * rows]
    second = weights[:, conv_width + temb_n : conv_width + 2 * temb_n]
    lifted = silu(silu(hidden[...] + bias_ref[...].T[:, 0:1])).astype(BF16)
    embedded = jnp.dot(second, lifted, preferred_element_type=F32)
    embedded = embedded[:, 0:1] + gains_ref[:, 5:6]
    set_moments(
        sums_ref[...], squares_ref[...], number, gains_ref[:, 0:1], EPS_BLOCK, mean, factor
    )
    normal_taps(start_ref, level, offset, mean, factor, breadth)
    block_n = min(512, token_n)
    for start in range(0, token_n, block_n):
        part = convolve(weights, level, offset, breadth, start, block_n)
        part = (part + embedded).astype(BF16)
        middle_ref[:, start : start + block_n] = part
        wide = part.astype(F32)
        if start == 0:
            sums_out[...] = lane_sums(wide)
            squares_out[...] = lane_sums(wide * wide)
        else:
            sums_out[...] += lane_sums(wide)
            squares_out[...] += lane_sums(wide * wide)


def second_kernel(
    counts,
    rows,
    breadth,
    origin_ref,
    space_ref,
    middle_ref,
    sums_ref,
    squares_ref,
    start_ref,
    gains_ref,
    *rest,
):
    pieces = rest[:counts]
    outputs = rest[counts : counts + 4]
    stage, weights, level, offset, mean, factor, sums, squares, block, tokens = rest[
        counts + 4 : counts + 14
    ]
    query_out, key_out, value_out = rest[counts + 14 : counts + 17]
    chan_n, token_n = middle_ref.shape
    query_n = query_out.shape[2]
    number = token_n * (chan_n // GROUPS)
    assemble(origin_ref, pieces, stage, rows, weights)
    conv_width = 9 * chan_n

    def small(index):
        base = conv_width + index * chan_n
        return weights[:, base : base + chan_n]

    set_moments(
        sums_ref[...], squares_ref[...], number, gains_ref[:, 1:2], EPS_BLOCK, mean, factor
    )
    normal_taps(middle_ref, level, offset, mean, factor, breadth)
    block_n = min(512, token_n)
    for start in range(0, token_n, block_n):
        part = convolve(weights, level, offset, breadth, start, block_n)
        part = (part + start_ref[:, start : start + block_n].astype(F32)).astype(BF16)
        block[:, start : start + block_n] = part
        wide = part.astype(F32)
        if start == 0:
            sums[...] = lane_sums(wide)
            squares[...] = lane_sums(wide * wide)
        else:
            sums[...] += lane_sums(wide)
            squares[...] += lane_sums(wide * wide)
    set_moments(sums[...], squares[...], number, gains_ref[:, 2:3], EPS_GROUP, mean, factor)
    own = pl.multiple_of(space_ref[0] * query_n, 128)

    def project(source):
        normed = ((source.astype(F32) - mean[:, 0:1]) * factor[:, 0:1]).astype(BF16)
        return jnp.dot(small(0), normed, preferred_element_type=F32)

    for start in range(0, token_n, block_n):
        projected = project(block[:, start : start + block_n])
        average = jnp.mean(projected, axis=0, keepdims=True)
        centred = projected - average
        spread = jnp.mean(centred * centred, axis=0, keepdims=True)
        scaled = centred * lax.rsqrt(spread + EPS_LAYER) * gains_ref[:, 4:5]
        token = scaled.astype(BF16)
        tokens[:, start : start + block_n] = token
        value = jnp.dot(small(3), token, preferred_element_type=F32)
        ones = jnp.ones((8, block_n), F32)
        for head in range(HEADS):
            piece = value[head * HEAD_SIZE : (head + 1) * HEAD_SIZE]
            value_out[head, :, start : start + block_n] = jnp.concatenate(
                [piece, ones], axis=0
            ).astype(BF16)
        upright = token.T
        half = HEADS // 2 * HEAD_SIZE
        for part in range(2):
            matrix = weights[
                part * half : (part + 1) * half,
                conv_width + 2 * chan_n : conv_width + 3 * chan_n,
            ]
            key_out[part, start : start + block_n, :] = lax.dot_general(
                upright, matrix, (((1,), (1,)), ((), ())), preferred_element_type=F32
            ).astype(BF16)
    query = jnp.dot(small(1), tokens[:, pl.ds(own, query_n)], preferred_element_type=F32)
    query = query * (math.log2(math.e) / math.sqrt(HEAD_SIZE))
    per_half = HEADS // 2
    for head in range(HEADS):
        spot = head % per_half
        piece = query[head * HEAD_SIZE : (head + 1) * HEAD_SIZE]
        parts = []
        if spot:
            parts.append(jnp.zeros((spot * HEAD_SIZE, query_n), F32))
        parts.append(piece)
        if spot < per_half - 1:
            parts.append(jnp.zeros(((per_half - 1 - spot) * HEAD_SIZE, query_n), F32))
        query_out[head] = jnp.concatenate(parts, axis=0).astype(BF16)
    attend(query_out, key_out, value_out, *rest[counts + 17 :])
    attended = rest[counts + 17]
    mine = block[:, pl.ds(own, query_n)]
    mixture = jnp.dot(small(4), attended[...].astype(BF16), preferred_element_type=F32)
    mixture = (mixture + project(mine)).astype(BF16)
    outer = jnp.dot(small(5), mixture, preferred_element_type=F32)
    report((mine.astype(F32) + outer).astype(BF16), breadth, space_ref[0] == 0, *outputs)


def exact_parts(value):
    high = value.astype(BF16)
    rest = value - high.astype(F32)
    middle = rest.astype(BF16)
    return [high, middle, (rest - middle.astype(F32)).astype(BF16)]


def attend(query_ref, key_ref, value_ref, attended, *slots):
    heads, _, query_n = query_ref.shape
    token_n = key_ref.shape[1]
    width = slots[0].shape[1]
    blocks = query_n // width
    items = heads * blocks
    key_n = min(256, token_n)

    def spot(item):
        return item // blocks, pl.multiple_of((item % blocks) * width, 128)

    def step(item, scores, tops, ahead, scores_ahead, tops_ahead):
        head_ahead, base_ahead = spot(ahead)
        query = query_ref[head_ahead, :, pl.ds(base_ahead, width)]
        running = mixed = None
        if item is not None:
            head, base = spot(item)
            top = jnp.max(tops[...], axis=0, keepdims=True)
        for start in range(0, token_n, key_n):
            keys = key_ref[head_ahead // (heads // 2), start : start + key_n, :]
            part = jnp.dot(keys, query, preferred_element_type=F32)
            scores_ahead[start : start + key_n, :] = part
            part = jnp.max(part.reshape(key_n // 8, 8, width), axis=0)
            running = part if running is None else jnp.maximum(running, part)
            if item is not None:
                weight = jnp.exp2(scores[start : start + key_n, :] - top).astype(BF16)
                part = jnp.dot(
                    value_ref[head, :, start : start + key_n], weight, preferred_element_type=F32
                )
                mixed = part if mixed is None else mixed + part
        tops_ahead[...] = running
        if item is not None:
            row = pl.multiple_of(head * HEAD_SIZE, 8)
            attended[pl.ds(row, HEAD_SIZE), pl.ds(base, width)] = (
                mixed[:HEAD_SIZE] / mixed[HEAD_SIZE : HEAD_SIZE + 1]
            )

    even, odd = slots[0:2], slots[2:4]
    step(None, None, None, 0, *even)

    def two(index, carry):
        step(2 * index, *even, 2 * index + 1, *odd)
        step(2 * index + 1, *odd, jnp.minimum(2 * index + 2, items - 1), *even)
        return carry

    lax.fori_loop(0, items // 2, two, 0)


def report(block_two, breadth, first, block_two_ref, sums_ref, squares_ref, packed_ref):
    query_n = block_two.shape[1]
    block_two_ref[...] = block_two
    wide = block_two.astype(F32)
    sums = lane_sums(wide)
    squares = lane_sums(wide * wide)
    sums_ref[...] = sums
    squares_ref[...] = squares
    edge = jnp.where(first, wide[:, query_n - breadth :], wide[:, :breadth])
    columns = exact_parts(jnp.sum(sums, axis=1, keepdims=True))
    columns += exact_parts(jnp.sum(squares, axis=1, keepdims=True))
    lane = lax.broadcasted_iota(jnp.int32, packed_ref.shape, 1)
    packed = jnp.zeros(packed_ref.shape, F32)
    for index, part in enumerate(columns):
        packed = jnp.where(lane == breadth + index, part.astype(F32), packed)
    packed_ref[...] = packed.astype(BF16)
    packed_ref[:, :breadth] = edge.astype(BF16)


def closing_kernel(
    breadth,
    number,
    space_n,
    space_ref,
    weight_ref,
    block_ref,
    above_ref,
    below_ref,
    sums_ref,
    squares_ref,
    gains_ref,
    kernel_ref,
    noise_ref,
    out_ref,
    active,
):
    chan_n, token_n = block_ref.shape
    lat_n = noise_ref.shape[1]
    sums, squares = sums_ref[...], squares_ref[...]
    if space_n == 2:
        lane = lax.broadcasted_iota(jnp.int32, sums.shape, 1)
        peer = above_ref[...].astype(F32)
        sums = sums + jnp.where((lane >= breadth) & (lane < breadth + 3), peer, 0.0)
        squares = squares + jnp.where((lane >= breadth + 3) & (lane < breadth + 6), peer, 0.0)
    mean, square = group_moments(sums, squares, number)
    factor = lax.rsqrt(square - mean * mean + EPS_BLOCK) * gains_ref[:, 3:4]

    def act(value):
        return silu((value.astype(F32) - mean) * factor)

    first = space_ref[0] == 0
    last = space_ref[0] == space_n - 1
    margin = 2 * breadth
    top = jnp.where(first, 0.0, act(above_ref[:, :breadth]))
    end = jnp.where(last, 0.0, act(below_ref[:, :breadth]))
    blank = jnp.zeros((chan_n, breadth), F32)
    active[:, :margin] = jnp.concatenate([blank, top], axis=1).astype(BF16)
    active[:, margin : margin + token_n] = act(block_ref[...]).astype(BF16)
    active[:, margin + token_n :] = jnp.concatenate([end, blank], axis=1).astype(BF16)
    taps = jnp.dot(kernel_ref[...], active[...], preferred_element_type=F32)
    total_n = token_n + 2 * margin
    lane = lax.broadcasted_iota(jnp.int32, (8, token_n), 1)
    column = lane % breadth
    result = jnp.zeros((8, token_n), F32)
    for offset in range(9):
        row_off, col_off = offset // 3 - 1, offset % 3 - 1
        piece = taps[offset * 8 : (offset + 1) * 8]
        shift = -(row_off * breadth + col_off) % total_n
        moved = pltpu.roll(piece, shift, 1) if shift else piece
        moved = moved[:, margin : margin + token_n]
        good = (column + col_off >= 0) & (column + col_off < breadth)
        result = result + jnp.where(good, moved, 0.0)
    weight = weight_ref[0]
    for row in range(token_n // breadth):
        part = result[0:lat_n, row * breadth : (row + 1) * breadth]
        out_ref[row] = weight * (part - noise_ref[row])


def kernel_call(body, out_shape, scratch, scalars=0):
    smem = pl.BlockSpec(memory_space=pltpu.SMEM)
    vmem = pl.BlockSpec(memory_space=pltpu.VMEM)

    def call(*args):
        return pl.pallas_call(
            body,
            out_shape=out_shape,
            in_specs=[smem] * scalars + [vmem] * (len(args) - scalars),
            scratch_shapes=scratch,
            compiler_params=pltpu.CompilerParams(vmem_limit_bytes=VMEM_BYTES),
        )(*args)

    return call


def body(
    latents,
    noise_draw,
    timesteps,
    inlet_conv,
    time_first,
    time_first_bias,
    time_second,
    time_second_bias,
    conv_first,
    conv_second,
    proj_inner,
    query_weight,
    key_weight,
    value_weight,
    attn_out,
    proj_outer,
    outlet_conv,
    first_gain,
    second_gain,
    third_gain,
    final_gain,
    layer_gain,
):
    shape = jax.ShapeDtypeStruct
    view_n, height, breadth, lat_n = latents.shape
    assert view_n == 1
    rows = conv_first.shape[1]
    chan_n = inlet_conv.shape[1]
    temb_n = time_first_bias.shape[0]
    many = temb_n // chan_n
    space_n = lax.axis_size("space")
    place = lax.axis_index("space")
    token_n = height * space_n * breadth
    query_n = height * breadth

    squares = (proj_inner, query_weight, key_weight, value_weight, attn_out, proj_outer)
    shards = (conv_first, time_first, time_second, conv_second) + squares
    conv_width = conv_first.shape[0]
    width_one = conv_width + 2 * temb_n
    width_two = conv_width + len(squares) * chan_n
    batch_one, batch_two = kernel_call(
        pack_kernel,
        [shape((rows, width_one), BF16), shape((rows, width_two), BF16)],
        [],
    )(*(shard.T for shard in shards))

    moments = [shape((chan_n, 128), F32)] * 2
    taps_n = 9 * lat_n
    taps_pad = -(-taps_n // 16) * 16
    alpha_bar = lookup(timesteps)

    def early():
        alpha_here = alpha_bar[:, None, None, None]
        noisy = jnp.sqrt(alpha_here) * latents + jnp.sqrt(1.0 - alpha_here) * noise_draw
        noisy = noisy.astype(BF16)[0].transpose(0, 2, 1)
        noisy = lax.all_gather(noisy, "space", axis=0, tiled=True)
        inlet = jnp.pad(inlet_conv.T, ((0, 0), (0, taps_pad - taps_n)))
        opened = kernel_call(
            lambda *refs: opening_kernel(breadth, *refs),
            [shape((chan_n, token_n), BF16)] + moments,
            [pltpu.VMEM((8, token_n), F32), pltpu.VMEM((taps_pad, token_n), F32)],
        )(noisy, inlet)
        wave = waveform_of(timesteps, chan_n // 2)
        wave = jnp.broadcast_to(wave.reshape(chan_n, 1), (chan_n, 128))
        gains = (first_gain, second_gain, third_gain, final_gain, layer_gain, time_second_bias)
        gains = jnp.stack(gains, axis=1)
        outlet = outlet_conv.T.reshape(lat_n, 9, chan_n).transpose(1, 0, 2)
        outlet = jnp.pad(outlet, ((0, 0), (0, 8 - lat_n), (0, 0))).reshape(72, chan_n)
        bias = jnp.broadcast_to(time_first_bias[None], (8, temb_n))
        return list(opened) + [wave, gains, outlet, bias]

    (pieces_one, pieces_two), origin, extra = gather_shards((batch_one, batch_two), early)
    start, sums, squares, wave, gains, outlet, bias = extra
    space_id = place.reshape(1).astype(jnp.int32)

    count_one = len(pieces_one)
    deep = sum(padded(piece.shape[0]) for piece in pieces_one)
    args = (origin, start, sums, squares, gains, wave, bias, *pieces_one)
    middle, sums, squares = kernel_call(
        lambda *refs: first_kernel(count_one, rows, breadth, *refs),
        [shape((chan_n, token_n), BF16)] + moments,
        [
            pltpu.VMEM((deep, width_one), BF16),
            pltpu.VMEM((chan_n, width_one), BF16),
            pltpu.VMEM((3 * chan_n, token_n), BF16),
            pltpu.VMEM((3 * chan_n, token_n + 2 * breadth), BF16),
            pltpu.VMEM((chan_n, 128), F32),
            pltpu.VMEM((chan_n, 128), F32),
            pltpu.VMEM((temb_n, 128), F32),
        ],
        1,
    )(*args)

    count_two = len(pieces_two)
    half = HEADS // 2 * HEAD_SIZE
    args = (origin, space_id, middle, sums, squares, start, gains, *pieces_two)
    width = min(512, query_n)
    block_two, sums, squares, packed = kernel_call(
        lambda *refs: second_kernel(count_two, rows, breadth, *refs),
        [shape((chan_n, query_n), BF16)] + moments + [shape((chan_n, 128), BF16)],
        [
            pltpu.VMEM((deep, width_two), BF16),
            pltpu.VMEM((chan_n, width_two), BF16),
            pltpu.VMEM((3 * chan_n, token_n), BF16),
            pltpu.VMEM((3 * chan_n, token_n + 2 * breadth), BF16),
            pltpu.VMEM((chan_n, 128), F32),
            pltpu.VMEM((chan_n, 128), F32),
            pltpu.VMEM((chan_n, 128), F32),
            pltpu.VMEM((chan_n, 128), F32),
            pltpu.VMEM((chan_n, token_n), BF16),
            pltpu.VMEM((chan_n, token_n), BF16),
            pltpu.VMEM((HEADS, half, query_n), BF16),
            pltpu.VMEM((2, token_n, half), BF16),
            pltpu.VMEM((HEADS, HEAD_SIZE + 8, token_n), BF16),
            pltpu.VMEM((chan_n, query_n), F32),
        ]
        + [pltpu.VMEM((token_n, width), F32), pltpu.VMEM((8, width), F32)] * 2,
        2,
    )(*args)

    if space_n == 2:
        above = below = lax.ppermute(packed, "space", [(0, 1), (1, 0)])
    else:
        sums, squares = lax.psum((sums, squares), "space")
        ahead = [(i, i + 1) for i in range(space_n - 1)]
        above = lax.ppermute(block_two[:, query_n - breadth :], "space", ahead)
        below = lax.ppermute(block_two[:, :breadth], "space", [(j, i) for i, j in ahead])
    number = token_n * (chan_n // GROUPS)
    args = (
        space_id,
        1.0 - alpha_bar,
        block_two,
        above,
        below,
        sums,
        squares,
        gains,
        outlet,
        noise_draw[0].transpose(0, 2, 1),
    )
    out = kernel_call(
        lambda *refs: closing_kernel(breadth, number, space_n, *refs),
        shape((height, lat_n, breadth), F32),
        [pltpu.VMEM((chan_n, query_n + 4 * breadth), BF16)],
        2,
    )(*args)
    return out.transpose(0, 2, 1)[None]


def solution(mesh):
    split = P(None, "batch")
    view = P("batch", "space", None, None)
    in_specs = (view, view, P("batch"), P(), split, P(), split, P())
    in_specs = in_specs + (split,) * 8 + (P(),) * 6
    return jax.shard_map(body, mesh=mesh, in_specs=in_specs, out_specs=view, check_vma=False)
```

```python
import math

import jax
import jax.numpy as jnp
from jax import lax
from jax.experimental import pallas as pl
from jax.experimental.pallas import tpu as pltpu
from jax.sharding import PartitionSpec as P


HEADS = 8
HEAD_SIZE = 40
GROUPS = 32
STEPS = 1000
EPS_GROUP = 1e-06
EPS_BLOCK = 1e-05
EPS_LAYER = 1e-05
VMEM_BYTES = 60 << 20
RING_LIMIT = 16
UNROLL = 2
F32 = jnp.float32
BF16 = jnp.bfloat16


def plan():
    fraction = jnp.arange(STEPS, dtype=F32) / (STEPS - 1)
    beta_root = math.sqrt(0.00085) + fraction * (math.sqrt(0.012) - math.sqrt(0.00085))
    return jnp.cumprod(1.0 - beta_root * beta_root)


def lookup(timesteps):
    matches = jnp.arange(STEPS, dtype=jnp.int32)[None, :] == timesteps[:, None]
    return jnp.sum(jnp.where(matches, plan()[None, :], 0.0), axis=1)


def waveform_of(timesteps, halfway):
    frequency = jnp.exp(-math.log(10000.0) * jnp.arange(halfway, dtype=F32) / halfway)
    angles = timesteps.astype(F32)[:, None] * frequency[None, :]
    return jnp.concatenate([jnp.cos(angles), jnp.sin(angles)], axis=1).astype(BF16)


def batch_ring(count):
    side = count // 4
    ring = 2 * side

    def group(spot):
        spot = spot % ring
        deep, wide = (spot, 0) if spot < side else (ring - 1 - spot, 1)
        return 2 * deep + wide

    onward = []
    for spot in range(ring):
        onward.append((2 * group(spot), 2 * group(spot + 1)))
        onward.append((2 * group(spot) + 1, 2 * group(spot - 1) + 1))
    sibling = [(place, place ^ 1) for place in range(count)]
    half = ring // 2
    spot_of = [0] * (count // 2)
    for spot in range(ring):
        spot_of[group(spot)] = spot
    table = []
    for place in range(count):
        core, spot = place % 2, spot_of[place // 2]
        row = [place, place ^ 1]
        step = -1 if core == 0 else 1
        for far in range(1, half):
            mine = group(spot + step * far)
            row += [2 * mine + core, 2 * mine + (core ^ 1)]
            theirs = group(spot - step * far)
            row += [2 * theirs + (core ^ 1), 2 * theirs + core]
        far_one = group(spot + step * half)
        row += [2 * far_one + core, 2 * far_one + (core ^ 1)]
        table.append(row)
    return onward, sibling, half, table


def gather_shards(urgent, patient, token, beside):
    count = lax.axis_size("batch")
    if count % 4 or count > RING_LIMIT:
        whole = [[lax.all_gather(part, "batch", axis=0, tiled=True)] for part in (urgent, patient)]
        return whole, jnp.arange(count, dtype=jnp.int32), [work(token) for work in beside]
    onward, sibling, half, table = batch_ring(count)
    rows = urgent.shape[0]
    others = [lax.ppermute(part, "batch", sibling) for part in (urgent, patient)]
    first, second, token = pair_up(token, (urgent, patient), others)
    origin = jnp.asarray(table, dtype=jnp.int32)[lax.axis_index("batch")]

    moving = first
    pieces_one = [moving]
    for _ in range(1, half):
        moving = lax.ppermute(moving, "batch", onward)
        pieces_one += [moving, lax.ppermute(moving, "batch", sibling)]
    last = lax.ppermute(moving[:rows], "batch", onward)
    pieces_one += [last, lax.ppermute(last, "batch", sibling)]

    moving = second
    pieces_two = [moving]
    extra = []
    for step in range(1, half):
        if step <= len(beside):
            now = (beside[step - 1](token), origin)
            moving, (now, origin) = lax.optimization_barrier((moving, now))
            extra.append(now)
        moving = lax.ppermute(moving, "batch", onward)
        pieces_two += [moving, lax.ppermute(moving, "batch", sibling)]
    extra += [work(token) for work in beside[half - 1 :]]
    pieces_two.append(lax.ppermute(moving, "batch", onward))
    return (pieces_one, pieces_two), origin, extra


def lane_sums(value):
    total = value[:, :128]
    for start in range(128, value.shape[1], 128):
        total = total + value[:, start : start + 128]
    return total


def exact_parts(value):
    high = value.astype(BF16).astype(F32)
    rest = value - high
    middle = rest.astype(BF16).astype(F32)
    return [high, middle, rest - middle]


def moment_columns(sums, squares, base):
    parts = exact_parts(jnp.sum(sums, axis=1, keepdims=True))
    parts += exact_parts(jnp.sum(squares, axis=1, keepdims=True))
    lane = lax.broadcasted_iota(jnp.int32, sums.shape, 1)
    columns = jnp.zeros(sums.shape, F32)
    for index, part in enumerate(parts):
        columns = jnp.where(lane == base + index, part, columns)
    return columns


def group_moments(columns, bases, number):
    chan_n = columns.shape[0]
    size = chan_n // GROUPS
    rows = lax.broadcasted_iota(jnp.int32, (chan_n, 1), 0) // size
    cols = lax.broadcasted_iota(jnp.int32, (1, chan_n), 1) // size
    member = jnp.where(rows == cols, 1.0, 0.0).astype(BF16)
    grouped = jnp.dot(member, columns.astype(BF16), preferred_element_type=F32)
    lane = lax.broadcasted_iota(jnp.int32, columns.shape, 1)
    totals = []
    for shift in (0, 3):
        keep = lane < 0
        for base in bases:
            keep = keep | ((lane >= base + shift) & (lane < base + shift + 3))
        kept = jnp.where(keep, grouped, 0.0)
        totals.append(jnp.sum(kept, axis=1, keepdims=True) / number)
    return totals


def padded(rows):
    return -(-rows // 16) * 16


def assemble(origin_ref, pieces, stage, rows, out_ref):
    total, deep = out_ref.shape[0], stage.shape[0]
    rid = lax.broadcasted_iota(jnp.int32, (total, deep), 0)
    cid = lax.broadcasted_iota(jnp.int32, (1, deep), 1)
    want = jnp.full((1, deep), -1, jnp.int32)
    place = base = 0
    for ref in pieces:
        size = ref.shape[0]
        stage[base : base + size, :] = ref[...]
        if padded(size) > size:
            fill = jnp.zeros((padded(size) - size, stage.shape[1]), stage.dtype)
            stage[base + size : base + padded(size), :] = fill
        for sub in range(size // rows):
            first = base + sub * rows
            inside = (cid >= first) & (cid < first + rows)
            want = jnp.where(inside, origin_ref[place] * rows + cid - first, want)
            place += 1
        base += padded(size)
    pick = jnp.where(rid == want, 1.0, 0.0).astype(BF16)
    width = stage.shape[1]
    for start in range(0, width, 512):
        stop = min(width, start + 512)
        out_ref[:, start:stop] = jnp.dot(
            pick, stage[:, start:stop], preferred_element_type=F32
        ).astype(BF16)


def spread_taps(load, level_ref, offset_ref, breadth, chunk=16):
    chan_n, token_n = level_ref.shape[0] // 3, level_ref.shape[1]

    def one(index, carry):
        base = pl.multiple_of(index * chunk, chunk)
        value = load(base, chunk)
        column = lax.broadcasted_iota(jnp.int32, (chunk, token_n), 1) % breadth
        left = jnp.where(column == 0, 0.0, pltpu.roll(value, 1, 1))
        right = jnp.where(column == breadth - 1, 0.0, pltpu.roll(value, token_n - 1, 1))
        margin = lax.broadcasted_iota(jnp.int32, (chunk, 2 * breadth), 1) < breadth
        for col, variant in enumerate((left, value, right)):
            place = pl.ds(pl.multiple_of(col * chan_n + base, chunk), chunk)
            level_ref[place, :] = variant.astype(BF16)
            later = pltpu.roll(variant, breadth, 1)
            head = later[:, : 2 * breadth]
            offset_ref[place, : 2 * breadth] = jnp.where(margin, 0.0, head).astype(BF16)
            offset_ref[place, 2 * breadth : token_n] = later[:, 2 * breadth :].astype(BF16)
            offset_ref[place, token_n:] = jnp.where(margin, head, 0.0).astype(BF16)
        return carry

    lax.fori_loop(0, chan_n // chunk, one, 0, unroll=UNROLL)


def convolve(weights, level_ref, offset_ref, breadth, start, block_n):
    deep = level_ref.shape[0]
    total = None
    for row in range(3):
        source = level_ref if row == 1 else offset_ref
        first = start + (2 * breadth if row == 2 else 0)
        part = jnp.dot(
            weights[:, row * deep : (row + 1) * deep],
            source[:, first : first + block_n],
            preferred_element_type=F32,
        )
        total = part if total is None else total + part
    return total


def silu(value):
    half = 0.5 * value
    return half + half * jnp.tanh(half)


def normal_taps(source_ref, level_ref, offset_ref, mean_ref, factor_ref, breadth):
    def load(base, chunk):
        value = source_ref[pl.ds(base, chunk), :].astype(F32)
        mean = mean_ref[pl.ds(base, chunk), 0:1]
        factor = factor_ref[pl.ds(base, chunk), 0:1]
        return silu((value - mean) * factor)

    spread_taps(load, level_ref, offset_ref, breadth)


def set_moments(sums, squares, number, gain, epsilon, mean_ref, factor_ref):
    mean, square = group_moments(moment_columns(sums, squares, 0), (0,), number)
    factor = lax.rsqrt(square - mean * mean + epsilon) * gain
    mean_ref[...] = jnp.broadcast_to(mean, mean_ref.shape)
    factor_ref[...] = jnp.broadcast_to(factor, factor_ref.shape)


def pair_kernel(token_ref, *refs):
    token_out, refs = refs[-1], refs[:-1]
    token_out[0] = token_ref[0]
    count = len(refs) // 3
    for index in range(count):
        one_ref, two_ref, out_ref = refs[index::count]
        rows = one_ref.shape[0]
        out_ref[:rows] = one_ref[...]
        out_ref[rows:] = two_ref[...]


def pair_up(token, ones, twos):
    wholes = [jax.ShapeDtypeStruct((2 * one.shape[0], one.shape[1]), one.dtype) for one in ones]
    smem = pl.BlockSpec(memory_space=pltpu.SMEM)
    vmem = pl.BlockSpec(memory_space=pltpu.VMEM)
    return pl.pallas_call(
        pair_kernel,
        out_shape=wholes + [jax.ShapeDtypeStruct(token.shape, token.dtype)],
        in_specs=[smem] + [vmem] * (2 * len(ones)),
        out_specs=[vmem] * len(ones) + [smem],
        compiler_params=pltpu.CompilerParams(vmem_limit_bytes=VMEM_BYTES),
    )(token, *ones, *twos)


def pack_kernel(conv_first, time_first, time_second, conv_second, *rest):
    squares, (one_ref, two_ref) = rest[:-2], rest[-2:]
    rows, conv_width = conv_first.shape
    chan_n = time_first.shape[1]
    one_ref[:, :conv_width] = conv_first[...]
    for index in range(time_first.shape[0] // rows):
        base = conv_width + index * chan_n
        one_ref[:, base : base + chan_n] = time_first[index * rows : (index + 1) * rows]
    one_ref[:, conv_width + time_second.shape[1] :] = time_second[...]
    two_ref[:, :conv_width] = conv_second[...]
    for index, square in enumerate(squares):
        base = conv_width + index * chan_n
        two_ref[:, base : base + chan_n] = square[...]


def opening_kernel(breadth, noisy_ref, kernel_ref, start_ref, sums_ref, squares_ref, flat, taps):
    height, lat_n, _ = noisy_ref.shape
    token_n = height * breadth
    flat[...] = jnp.zeros(flat.shape, F32)
    for row in range(height):
        flat[0:lat_n, row * breadth : (row + 1) * breadth] = noisy_ref[row].astype(F32)
    taps[...] = jnp.zeros(taps.shape, F32)
    value = flat[...]
    lane = lax.broadcasted_iota(jnp.int32, value.shape, 1)
    column = lane % breadth
    for offset in range(9):
        row_off, col_off = offset // 3 - 1, offset % 3 - 1
        shift = -(row_off * breadth + col_off) % token_n
        moved = pltpu.roll(value, shift, 1) if shift else value
        good = (column + col_off >= 0) & (column + col_off < breadth)
        good = good & (lane + row_off * breadth >= 0) & (lane + row_off * breadth < token_n)
        moved = jnp.where(good, moved, 0.0)
        taps[offset * lat_n : (offset + 1) * lat_n, :] = moved[0:lat_n]
    block_n = min(512, token_n)
    for start in range(0, token_n, block_n):
        part = jnp.dot(
            kernel_ref[...],
            taps[:, start : start + block_n].astype(BF16),
            preferred_element_type=F32,
        ).astype(BF16)
        start_ref[:, start : start + block_n] = part
        wide = part.astype(F32)
        if start == 0:
            sums_ref[...] = lane_sums(wide)
            squares_ref[...] = lane_sums(wide * wide)
        else:
            sums_ref[...] += lane_sums(wide)
            squares_ref[...] += lane_sums(wide * wide)


def first_kernel(
    counts,
    rows,
    breadth,
    origin_ref,
    start_ref,
    sums_ref,
    squares_ref,
    gains_ref,
    wave_ref,
    bias_ref,
    *rest,
):
    pieces = rest[:counts]
    middle_ref, sums_out, squares_out = rest[counts : counts + 3]
    stage, weights, level, offset, mean, factor, hidden = rest[counts + 3 :]
    chan_n, token_n = start_ref.shape
    gains = gains_ref[...].T
    number = token_n * (chan_n // GROUPS)
    assemble(origin_ref, pieces, stage, rows, weights)
    conv_width = 9 * chan_n
    temb_n = hidden.shape[0]
    many = temb_n // chan_n
    for index in range(many):
        first = weights[:, conv_width + index * chan_n : conv_width + (index + 1) * chan_n]
        inner = jnp.dot(first, wave_ref[...], preferred_element_type=F32)
        for place in range(chan_n // rows):
            base = place * many * rows + index * rows
            hidden[base : base + rows, :] = inner[place * rows : (place + 1) * rows]
    second = weights[:, conv_width + temb_n : conv_width + 2 * temb_n]
    lifted = silu(silu(hidden[...] + bias_ref[...].T[:, 0:1])).astype(BF16)
    embedded = jnp.dot(second, lifted, preferred_element_type=F32)
    embedded = embedded[:, 0:1] + gains[:, 5:6]
    set_moments(
        sums_ref[...], squares_ref[...], number, gains[:, 0:1], EPS_BLOCK, mean, factor
    )
    normal_taps(start_ref, level, offset, mean, factor, breadth)
    block_n = min(512, token_n)
    for start in range(0, token_n, block_n):
        part = convolve(weights, level, offset, breadth, start, block_n)
        part = (part + embedded).astype(BF16)
        middle_ref[:, start : start + block_n] = part
        wide = part.astype(F32)
        if start == 0:
            sums_out[...] = lane_sums(wide)
            squares_out[...] = lane_sums(wide * wide)
        else:
            sums_out[...] += lane_sums(wide)
            squares_out[...] += lane_sums(wide * wide)


def second_kernel(
    counts,
    rows,
    breadth,
    origin_ref,
    space_ref,
    middle_ref,
    sums_ref,
    squares_ref,
    start_ref,
    gains_ref,
    *rest,
):
    pieces = rest[:counts]
    outputs = rest[counts : counts + 4]
    stage, weights, level, offset, mean, factor, sums, squares, block, tokens = rest[
        counts + 4 : counts + 14
    ]
    query_out, key_out, value_out = rest[counts + 14 : counts + 17]
    chan_n, token_n = middle_ref.shape
    gains = gains_ref[...].T
    query_n = query_out.shape[2]
    number = token_n * (chan_n // GROUPS)
    assemble(origin_ref, pieces, stage, rows, weights)
    conv_width = 9 * chan_n

    def small(index):
        base = conv_width + index * chan_n
        return weights[:, base : base + chan_n]

    set_moments(
        sums_ref[...], squares_ref[...], number, gains[:, 1:2], EPS_BLOCK, mean, factor
    )
    normal_taps(middle_ref, level, offset, mean, factor, breadth)
    block_n = min(512, token_n)
    for start in range(0, token_n, block_n):
        part = convolve(weights, level, offset, breadth, start, block_n)
        part = (part + start_ref[:, start : start + block_n].astype(F32)).astype(BF16)
        block[:, start : start + block_n] = part
        wide = part.astype(F32)
        if start == 0:
            sums[...] = lane_sums(wide)
            squares[...] = lane_sums(wide * wide)
        else:
            sums[...] += lane_sums(wide)
            squares[...] += lane_sums(wide * wide)
    set_moments(sums[...], squares[...], number, gains[:, 2:3], EPS_GROUP, mean, factor)
    own = pl.multiple_of(space_ref[0] * query_n, 128)

    def project(source):
        normed = ((source.astype(F32) - mean[:, 0:1]) * factor[:, 0:1]).astype(BF16)
        return jnp.dot(small(0), normed, preferred_element_type=F32)

    for start in range(0, token_n, block_n):
        projected = project(block[:, start : start + block_n])
        average = jnp.mean(projected, axis=0, keepdims=True)
        centred = projected - average
        spread = jnp.mean(centred * centred, axis=0, keepdims=True)
        scaled = centred * lax.rsqrt(spread + EPS_LAYER) * gains[:, 4:5]
        token = scaled.astype(BF16)
        tokens[:, start : start + block_n] = token
        value = jnp.dot(small(3), token, preferred_element_type=F32)
        ones = jnp.ones((8, block_n), F32)
        for head in range(HEADS):
            piece = value[head * HEAD_SIZE : (head + 1) * HEAD_SIZE]
            value_out[head, :, start : start + block_n] = jnp.concatenate(
                [piece, ones], axis=0
            ).astype(BF16)
        upright = token.T
        half = HEADS // 2 * HEAD_SIZE
        for part in range(2):
            matrix = weights[
                part * half : (part + 1) * half,
                conv_width + 2 * chan_n : conv_width + 3 * chan_n,
            ]
            key_out[part, start : start + block_n, :] = lax.dot_general(
                upright, matrix, (((1,), (1,)), ((), ())), preferred_element_type=F32
            ).astype(BF16)
    query = jnp.dot(small(1), tokens[:, pl.ds(own, query_n)], preferred_element_type=F32)
    query = query * (math.log2(math.e) / math.sqrt(HEAD_SIZE))
    per_half = HEADS // 2
    for head in range(HEADS):
        spot = head % per_half
        piece = query[head * HEAD_SIZE : (head + 1) * HEAD_SIZE]
        parts = []
        if spot:
            parts.append(jnp.zeros((spot * HEAD_SIZE, query_n), F32))
        parts.append(piece)
        if spot < per_half - 1:
            parts.append(jnp.zeros(((per_half - 1 - spot) * HEAD_SIZE, query_n), F32))
        query_out[head] = jnp.concatenate(parts, axis=0).astype(BF16)
    attend(query_out, key_out, value_out, *rest[counts + 17 :])
    attended = rest[counts + 17]
    mine = block[:, pl.ds(own, query_n)]
    mixture = jnp.dot(small(4), attended[...].astype(BF16), preferred_element_type=F32)
    mixture = (mixture + project(mine)).astype(BF16)
    outer = jnp.dot(small(5), mixture, preferred_element_type=F32)
    report((mine.astype(F32) + outer).astype(BF16), breadth, space_ref[0] == 0, *outputs)


def attend(query_ref, key_ref, value_ref, attended, *slots):
    heads, _, query_n = query_ref.shape
    token_n = key_ref.shape[1]
    width = slots[0].shape[1]
    blocks = query_n // width
    items = heads * blocks
    key_n = min(256, token_n)

    def spot(item):
        return item // blocks, pl.multiple_of((item % blocks) * width, 128)

    def step(item, scores, tops, ahead, scores_ahead, tops_ahead):
        head_ahead, base_ahead = spot(ahead)
        query = query_ref[head_ahead, :, pl.ds(base_ahead, width)]
        running = mixed = None
        if item is not None:
            head, base = spot(item)
            top = jnp.max(tops[...], axis=0, keepdims=True)
        for start in range(0, token_n, key_n):
            keys = key_ref[head_ahead // (heads // 2), start : start + key_n, :]
            part = jnp.dot(keys, query, preferred_element_type=F32)
            scores_ahead[start : start + key_n, :] = part
            part = jnp.max(part.reshape(key_n // 8, 8, width), axis=0)
            running = part if running is None else jnp.maximum(running, part)
            if item is not None:
                weight = jnp.exp2(scores[start : start + key_n, :] - top).astype(BF16)
                part = jnp.dot(
                    value_ref[head, :, start : start + key_n], weight, preferred_element_type=F32
                )
                mixed = part if mixed is None else mixed + part
        tops_ahead[...] = running
        if item is not None:
            row = pl.multiple_of(head * HEAD_SIZE, 8)
            attended[pl.ds(row, HEAD_SIZE), pl.ds(base, width)] = (
                mixed[:HEAD_SIZE] / mixed[HEAD_SIZE : HEAD_SIZE + 1]
            )

    even, odd = slots[0:2], slots[2:4]
    step(None, None, None, 0, *even)

    def two(index, carry):
        step(2 * index, *even, 2 * index + 1, *odd)
        step(2 * index + 1, *odd, jnp.minimum(2 * index + 2, items - 1), *even)
        return carry

    lax.fori_loop(0, items // 2, two, 0)


def report(block_two, breadth, first, block_two_ref, sums_ref, squares_ref, packed_ref):
    query_n = block_two.shape[1]
    block_two_ref[...] = block_two
    wide = block_two.astype(F32)
    sums = lane_sums(wide)
    squares = lane_sums(wide * wide)
    sums_ref[...] = sums
    squares_ref[...] = squares
    edge = jnp.where(first, wide[:, query_n - breadth :], wide[:, :breadth])
    packed_ref[...] = moment_columns(sums, squares, breadth).astype(BF16)
    packed_ref[:, :breadth] = edge.astype(BF16)


def closing_kernel(
    breadth,
    number,
    space_n,
    space_ref,
    weight_ref,
    block_ref,
    above_ref,
    below_ref,
    sums_ref,
    squares_ref,
    gains_ref,
    kernel_ref,
    noise_ref,
    out_ref,
    active,
):
    chan_n, token_n = block_ref.shape
    gains = gains_ref[...].T
    lat_n = noise_ref.shape[1]
    columns = moment_columns(sums_ref[...], squares_ref[...], 0)
    bases = (0,)
    if space_n == 2:
        lane = lax.broadcasted_iota(jnp.int32, columns.shape, 1)
        columns = jnp.where(lane >= breadth, above_ref[...].astype(F32), columns)
        bases = (0, breadth)
    mean, square = group_moments(columns, bases, number)
    factor = lax.rsqrt(square - mean * mean + EPS_BLOCK) * gains[:, 3:4]

    def act(value):
        return silu((value.astype(F32) - mean) * factor)

    first = space_ref[0] == 0
    last = space_ref[0] == space_n - 1
    margin = 2 * breadth
    top = jnp.where(first, 0.0, act(above_ref[:, :breadth]))
    end = jnp.where(last, 0.0, act(below_ref[:, :breadth]))
    blank = jnp.zeros((chan_n, breadth), F32)
    active[:, :margin] = jnp.concatenate([blank, top], axis=1).astype(BF16)
    active[:, margin : margin + token_n] = act(block_ref[...]).astype(BF16)
    active[:, margin + token_n :] = jnp.concatenate([end, blank], axis=1).astype(BF16)
    taps = jnp.dot(kernel_ref[...], active[...], preferred_element_type=F32)
    total_n = token_n + 2 * margin
    lane = lax.broadcasted_iota(jnp.int32, (8, token_n), 1)
    column = lane % breadth
    result = jnp.zeros((8, token_n), F32)
    for offset in range(9):
        row_off, col_off = offset // 3 - 1, offset % 3 - 1
        piece = taps[offset * 8 : (offset + 1) * 8]
        shift = -(row_off * breadth + col_off) % total_n
        moved = pltpu.roll(piece, shift, 1) if shift else piece
        moved = moved[:, margin : margin + token_n]
        good = (column + col_off >= 0) & (column + col_off < breadth)
        result = result + jnp.where(good, moved, 0.0)
    weight = weight_ref[0]
    for row in range(token_n // breadth):
        part = result[0:lat_n, row * breadth : (row + 1) * breadth]
        out_ref[row] = weight * (part - noise_ref[row])


def kernel_call(body, out_shape, scratch, scalars=0, flops=0):
    smem = pl.BlockSpec(memory_space=pltpu.SMEM)
    vmem = pl.BlockSpec(memory_space=pltpu.VMEM)
    cost = pl.CostEstimate(flops=flops, transcendentals=0, bytes_accessed=0) if flops else None

    def call(*args):
        return pl.pallas_call(
            body,
            out_shape=out_shape,
            in_specs=[smem] * scalars + [vmem] * (len(args) - scalars),
            scratch_shapes=scratch,
            compiler_params=pltpu.CompilerParams(vmem_limit_bytes=VMEM_BYTES),
            cost_estimate=cost,
        )(*args)

    return call


def body(
    latents,
    noise_draw,
    timesteps,
    inlet_conv,
    time_first,
    time_first_bias,
    time_second,
    time_second_bias,
    conv_first,
    conv_second,
    proj_inner,
    query_weight,
    key_weight,
    value_weight,
    attn_out,
    proj_outer,
    outlet_conv,
    first_gain,
    second_gain,
    third_gain,
    final_gain,
    layer_gain,
):
    shape = jax.ShapeDtypeStruct
    view_n, height, breadth, lat_n = latents.shape
    assert view_n == 1
    rows = conv_first.shape[1]
    chan_n = inlet_conv.shape[1]
    temb_n = time_first_bias.shape[0]
    space_n = lax.axis_size("space")
    place = lax.axis_index("space")
    token_n = height * space_n * breadth
    query_n = height * breadth

    squares = (proj_inner, query_weight, key_weight, value_weight, attn_out, proj_outer)
    shards = (conv_first, time_first, time_second, conv_second) + squares
    conv_width = conv_first.shape[0]
    width_one = conv_width + 2 * temb_n
    width_two = conv_width + len(squares) * chan_n
    batch_one, batch_two = kernel_call(
        pack_kernel,
        [shape((rows, width_one), BF16), shape((rows, width_two), BF16)],
        [],
    )(*(shard.T for shard in shards))

    moments = [shape((chan_n, 128), F32)] * 2
    taps_n = 9 * lat_n
    taps_pad = -(-taps_n // 16) * 16

    def early(steps):
        alpha_bar = lookup(steps)
        alpha_here = alpha_bar[:, None, None, None]
        noisy = jnp.sqrt(alpha_here) * latents + jnp.sqrt(1.0 - alpha_here) * noise_draw
        noisy = noisy.astype(BF16)[0].transpose(0, 2, 1)
        if space_n == 2:
            other = lax.ppermute(noisy, "space", [(0, 1), (1, 0)])
            noisy = jnp.stack([noisy, other])
            noisy = jnp.where(place == 0, noisy, noisy[::-1]).reshape(2 * height, lat_n, breadth)
        else:
            noisy = lax.all_gather(noisy, "space", axis=0, tiled=True)
        inlet = jnp.pad(inlet_conv.T, ((0, 0), (0, taps_pad - taps_n)))
        opened = kernel_call(
            lambda *refs: opening_kernel(breadth, *refs),
            [shape((chan_n, token_n), BF16)] + moments,
            [pltpu.VMEM((8, token_n), F32), pltpu.VMEM((taps_pad, token_n), F32)],
        )(noisy, inlet)
        return opened, alpha_bar

    def later(steps):
        wave = waveform_of(steps, chan_n // 2)
        wave = jnp.broadcast_to(wave.reshape(chan_n, 1), (chan_n, 128))
        gains = (first_gain, second_gain, third_gain, final_gain, layer_gain, time_second_bias)
        gains = jnp.stack(gains + (layer_gain,) * 2)
        outlet = outlet_conv.T.reshape(lat_n, 9, chan_n).transpose(1, 0, 2)
        outlet = jnp.pad(outlet, ((0, 0), (0, 8 - lat_n), (0, 0))).reshape(72, chan_n)
        bias = jnp.broadcast_to(time_first_bias[None], (8, temb_n))
        return wave, gains, outlet, bias

    (pieces_one, pieces_two), origin, extra = gather_shards(
        batch_one, batch_two, timesteps, (early, later)
    )
    ((start, sums, squares), alpha_bar), (wave, gains, outlet, bias) = extra
    space_id = place.reshape(1).astype(jnp.int32)

    count_one = len(pieces_one)
    deep = sum(padded(piece.shape[0]) for piece in pieces_one)
    deep_two = sum(padded(piece.shape[0]) for piece in pieces_two)
    args = (origin, start, sums, squares, gains, wave, bias, *pieces_one)
    middle, sums, squares = kernel_call(
        lambda *refs: first_kernel(count_one, rows, breadth, *refs),
        [shape((chan_n, token_n), BF16)] + moments,
        [
            pltpu.VMEM((deep, width_one), BF16),
            pltpu.VMEM((chan_n, width_one), BF16),
            pltpu.VMEM((3 * chan_n, token_n), BF16),
            pltpu.VMEM((3 * chan_n, token_n + 2 * breadth), BF16),
            pltpu.VMEM((chan_n, 128), F32),
            pltpu.VMEM((chan_n, 128), F32),
            pltpu.VMEM((temb_n, 128), F32),
        ],
        1,
        2 * token_n * conv_width * chan_n,
    )(*args)

    count_two = len(pieces_two)
    half = HEADS // 2 * HEAD_SIZE
    args = (origin, space_id, middle, sums, squares, start, gains, *pieces_two)
    width = min(512, query_n)
    block_two, sums, squares, packed = kernel_call(
        lambda *refs: second_kernel(count_two, rows, breadth, *refs),
        [shape((chan_n, query_n), BF16)] + moments + [shape((chan_n, 128), BF16)],
        [
            pltpu.VMEM((deep_two, width_two), BF16),
            pltpu.VMEM((chan_n, width_two), BF16),
            pltpu.VMEM((3 * chan_n, token_n), BF16),
            pltpu.VMEM((3 * chan_n, token_n + 2 * breadth), BF16),
            pltpu.VMEM((chan_n, 128), F32),
            pltpu.VMEM((chan_n, 128), F32),
            pltpu.VMEM((chan_n, 128), F32),
            pltpu.VMEM((chan_n, 128), F32),
            pltpu.VMEM((chan_n, token_n), BF16),
            pltpu.VMEM((chan_n, token_n), BF16),
            pltpu.VMEM((HEADS, half, query_n), BF16),
            pltpu.VMEM((2, token_n, half), BF16),
            pltpu.VMEM((HEADS, HEAD_SIZE + 8, token_n), BF16),
            pltpu.VMEM((chan_n, query_n), F32),
        ]
        + [pltpu.VMEM((token_n, width), F32), pltpu.VMEM((8, width), F32)] * 2,
        2,
    )(*args)

    if space_n == 2:
        above = below = lax.ppermute(packed, "space", [(0, 1), (1, 0)])
    else:
        sums, squares = lax.psum((sums, squares), "space")
        ahead = [(i, i + 1) for i in range(space_n - 1)]
        above = lax.ppermute(block_two[:, query_n - breadth :], "space", ahead)
        below = lax.ppermute(block_two[:, :breadth], "space", [(j, i) for i, j in ahead])
    number = token_n * (chan_n // GROUPS)
    args = (
        space_id,
        1.0 - alpha_bar,
        block_two,
        above,
        below,
        sums,
        squares,
        gains,
        outlet,
        noise_draw[0].transpose(0, 2, 1),
    )
    out = kernel_call(
        lambda *refs: closing_kernel(breadth, number, space_n, *refs),
        shape((height, lat_n, breadth), F32),
        [pltpu.VMEM((chan_n, query_n + 4 * breadth), BF16)],
        2,
    )(*args)
    return out.transpose(0, 2, 1)[None]


def solution(mesh):
    split = P(None, "batch")
    view = P("batch", "space", None, None)
    in_specs = (view, view, P("batch"), P(), split, P(), split, P())
    in_specs = in_specs + (split,) * 8 + (P(),) * 6

    return jax.shard_map(body, mesh=mesh, in_specs=in_specs, out_specs=view, check_vma=False)
```

```python
import math

import jax
import jax.numpy as jnp
from jax import lax
from jax.experimental import pallas as pl
from jax.experimental.pallas import tpu as pltpu
from jax.sharding import PartitionSpec as P


HEADS = 8
HEAD_SIZE = 40
GROUPS = 32
STEPS = 1000
EPS_GROUP = 1e-06
EPS_BLOCK = 1e-05
EPS_LAYER = 1e-05
VMEM_BYTES = 60 << 20
RING_LIMIT = 16
UNROLL = 2
F32 = jnp.float32
BF16 = jnp.bfloat16


def plan():
    fraction = jnp.arange(STEPS, dtype=F32) / (STEPS - 1)
    beta_root = math.sqrt(0.00085) + fraction * (math.sqrt(0.012) - math.sqrt(0.00085))
    return jnp.cumprod(1.0 - beta_root * beta_root)


def lookup(timesteps):
    matches = jnp.arange(STEPS, dtype=jnp.int32)[None, :] == timesteps[:, None]
    return jnp.sum(jnp.where(matches, plan()[None, :], 0.0), axis=1)


def waveform_of(timesteps, halfway):
    frequency = jnp.exp(-math.log(10000.0) * jnp.arange(halfway, dtype=F32) / halfway)
    angles = timesteps.astype(F32)[:, None] * frequency[None, :]
    return jnp.concatenate([jnp.cos(angles), jnp.sin(angles)], axis=1).astype(BF16)


def batch_ring(count):
    side = count // 4
    ring = 2 * side

    def group(spot):
        spot = spot % ring
        deep, wide = (spot, 0) if spot < side else (ring - 1 - spot, 1)
        return 2 * deep + wide

    onward = []
    for spot in range(ring):
        onward.append((2 * group(spot), 2 * group(spot + 1)))
        onward.append((2 * group(spot) + 1, 2 * group(spot - 1) + 1))
    sibling = [(place, place ^ 1) for place in range(count)]
    half = ring // 2
    spot_of = [0] * (count // 2)
    for spot in range(ring):
        spot_of[group(spot)] = spot
    table = []
    for place in range(count):
        core, spot = place % 2, spot_of[place // 2]
        row = [place, place ^ 1]
        step = -1 if core == 0 else 1
        for far in range(1, half):
            mine = group(spot + step * far)
            row += [2 * mine + core, 2 * mine + (core ^ 1)]
            theirs = group(spot - step * far)
            row += [2 * theirs + (core ^ 1), 2 * theirs + core]
        far_one = group(spot + step * half)
        row += [2 * far_one + core, 2 * far_one + (core ^ 1)]
        table.append(row)
    return onward, sibling, half, table


def gather_shards(urgent, patient, token, beside):
    count = lax.axis_size("batch")
    if count % 4 or count > RING_LIMIT:
        whole = [[lax.all_gather(part, "batch", axis=0, tiled=True)] for part in (urgent, patient)]
        return whole, jnp.arange(count, dtype=jnp.int32), [work(token) for work in beside]
    onward, sibling, half, table = batch_ring(count)
    rows = urgent.shape[0]
    others = [lax.ppermute(part, "batch", sibling) for part in (urgent, patient)]
    first, second, token = pair_up(token, (urgent, patient), others)
    origin = jnp.asarray(table, dtype=jnp.int32)[lax.axis_index("batch")]

    moving = first
    pieces_one = [moving]
    for _ in range(1, half):
        moving = lax.ppermute(moving, "batch", onward)
        pieces_one += [moving, lax.ppermute(moving, "batch", sibling)]
    last = lax.ppermute(moving[:rows], "batch", onward)
    pieces_one += [last, lax.ppermute(last, "batch", sibling)]

    moving = second
    pieces_two = [moving]
    extra = []
    for step in range(1, half):
        if 1 < step <= len(beside) + 1:
            moving, now = lax.optimization_barrier((moving, beside[step - 2](token)))
            extra.append(now)
        moving = lax.ppermute(moving, "batch", onward)
        pieces_two += [moving, lax.ppermute(moving, "batch", sibling)]
    extra += [work(token) for work in beside[max(half - 2, 0) :]]
    pieces_two.append(lax.ppermute(moving, "batch", onward))
    return (pieces_one, pieces_two), origin, extra


def lane_sums(value):
    total = value[:, :128]
    for start in range(128, value.shape[1], 128):
        total = total + value[:, start : start + 128]
    return total


def exact_parts(value):
    high = value.astype(BF16).astype(F32)
    rest = value - high
    middle = rest.astype(BF16).astype(F32)
    return [high, middle, rest - middle]


def moment_columns(sums, squares, base):
    parts = exact_parts(jnp.sum(sums, axis=1, keepdims=True))
    parts += exact_parts(jnp.sum(squares, axis=1, keepdims=True))
    lane = lax.broadcasted_iota(jnp.int32, sums.shape, 1)
    columns = jnp.zeros(sums.shape, F32)
    for index, part in enumerate(parts):
        columns = jnp.where(lane == base + index, part, columns)
    return columns


def group_moments(columns, bases, number):
    chan_n = columns.shape[0]
    size = chan_n // GROUPS
    rows = lax.broadcasted_iota(jnp.int32, (chan_n, 1), 0) // size
    cols = lax.broadcasted_iota(jnp.int32, (1, chan_n), 1) // size
    member = jnp.where(rows == cols, 1.0, 0.0).astype(BF16)
    grouped = jnp.dot(member, columns.astype(BF16), preferred_element_type=F32)
    lane = lax.broadcasted_iota(jnp.int32, columns.shape, 1)
    totals = []
    for shift in (0, 3):
        keep = lane < 0
        for base in bases:
            keep = keep | ((lane >= base + shift) & (lane < base + shift + 3))
        kept = jnp.where(keep, grouped, 0.0)
        totals.append(jnp.sum(kept, axis=1, keepdims=True) / number)
    return totals


def padded(rows):
    return -(-rows // 16) * 16


def assemble(origin_ref, pieces, stage, rows, out_ref):
    total, deep = out_ref.shape[0], stage.shape[0]
    rid = lax.broadcasted_iota(jnp.int32, (total, deep), 0)
    cid = lax.broadcasted_iota(jnp.int32, (1, deep), 1)
    want = jnp.full((1, deep), -1, jnp.int32)
    place = base = 0
    for ref in pieces:
        size = ref.shape[0]
        stage[base : base + size, :] = ref[...]
        if padded(size) > size:
            fill = jnp.zeros((padded(size) - size, stage.shape[1]), stage.dtype)
            stage[base + size : base + padded(size), :] = fill
        for sub in range(size // rows):
            first = base + sub * rows
            inside = (cid >= first) & (cid < first + rows)
            want = jnp.where(inside, origin_ref[place] * rows + cid - first, want)
            place += 1
        base += padded(size)
    pick = jnp.where(rid == want, 1.0, 0.0).astype(BF16)
    width = stage.shape[1]
    for start in range(0, width, 512):
        stop = min(width, start + 512)
        out_ref[:, start:stop] = jnp.dot(
            pick, stage[:, start:stop], preferred_element_type=F32
        ).astype(BF16)


def spread_taps(load, level_ref, offset_ref, breadth, chunk=16):
    chan_n, token_n = level_ref.shape[0] // 3, level_ref.shape[1]

    def one(index, carry):
        base = pl.multiple_of(index * chunk, chunk)
        value = load(base, chunk)
        column = lax.broadcasted_iota(jnp.int32, (chunk, token_n), 1) % breadth
        left = jnp.where(column == 0, 0.0, pltpu.roll(value, 1, 1))
        right = jnp.where(column == breadth - 1, 0.0, pltpu.roll(value, token_n - 1, 1))
        margin = lax.broadcasted_iota(jnp.int32, (chunk, 2 * breadth), 1) < breadth
        for col, variant in enumerate((left, value, right)):
            place = pl.ds(pl.multiple_of(col * chan_n + base, chunk), chunk)
            level_ref[place, :] = variant.astype(BF16)
            later = pltpu.roll(variant, breadth, 1)
            head = later[:, : 2 * breadth]
            offset_ref[place, : 2 * breadth] = jnp.where(margin, 0.0, head).astype(BF16)
            offset_ref[place, 2 * breadth : token_n] = later[:, 2 * breadth :].astype(BF16)
            offset_ref[place, token_n:] = jnp.where(margin, head, 0.0).astype(BF16)
        return carry

    lax.fori_loop(0, chan_n // chunk, one, 0, unroll=UNROLL)


def convolve(weights, level_ref, offset_ref, breadth, start, block_n):
    deep = level_ref.shape[0]
    total = None
    for row in range(3):
        source = level_ref if row == 1 else offset_ref
        first = start + (2 * breadth if row == 2 else 0)
        part = jnp.dot(
            weights[:, row * deep : (row + 1) * deep],
            source[:, first : first + block_n],
            preferred_element_type=F32,
        )
        total = part if total is None else total + part
    return total


def silu(value):
    half = 0.5 * value
    return half + half * jnp.tanh(half)


def normal_taps(source_ref, level_ref, offset_ref, mean_ref, factor_ref, breadth):
    def load(base, chunk):
        value = source_ref[pl.ds(base, chunk), :].astype(F32)
        mean = mean_ref[pl.ds(base, chunk), 0:1]
        factor = factor_ref[pl.ds(base, chunk), 0:1]
        return silu((value - mean) * factor)

    spread_taps(load, level_ref, offset_ref, breadth)


def set_moments(sums, squares, number, gain, epsilon, mean_ref, factor_ref):
    mean, square = group_moments(moment_columns(sums, squares, 0), (0,), number)
    factor = lax.rsqrt(square - mean * mean + epsilon) * gain
    mean_ref[...] = jnp.broadcast_to(mean, mean_ref.shape)
    factor_ref[...] = jnp.broadcast_to(factor, factor_ref.shape)


def pair_kernel(token_ref, *refs):
    token_out, refs = refs[-1], refs[:-1]
    token_out[0] = token_ref[0]
    count = len(refs) // 3
    for index in range(count):
        one_ref, two_ref, out_ref = refs[index::count]
        rows = one_ref.shape[0]
        out_ref[:rows] = one_ref[...]
        out_ref[rows:] = two_ref[...]


def pair_up(token, ones, twos):
    wholes = [jax.ShapeDtypeStruct((2 * one.shape[0], one.shape[1]), one.dtype) for one in ones]
    smem = pl.BlockSpec(memory_space=pltpu.SMEM)
    vmem = pl.BlockSpec(memory_space=pltpu.VMEM)
    return pl.pallas_call(
        pair_kernel,
        out_shape=wholes + [jax.ShapeDtypeStruct(token.shape, token.dtype)],
        in_specs=[smem] + [vmem] * (2 * len(ones)),
        out_specs=[vmem] * len(ones) + [smem],
        compiler_params=pltpu.CompilerParams(vmem_limit_bytes=VMEM_BYTES),
    )(token, *ones, *twos)


def pack_kernel(conv_first, time_first, time_second, conv_second, *rest):
    squares, (one_ref, two_ref) = rest[:-2], rest[-2:]
    rows, conv_width = conv_first.shape
    chan_n = time_first.shape[1]
    one_ref[:, :conv_width] = conv_first[...]
    for index in range(time_first.shape[0] // rows):
        base = conv_width + index * chan_n
        one_ref[:, base : base + chan_n] = time_first[index * rows : (index + 1) * rows]
    one_ref[:, conv_width + time_second.shape[1] :] = time_second[...]
    two_ref[:, :conv_width] = conv_second[...]
    for index, square in enumerate(squares):
        base = conv_width + index * chan_n
        two_ref[:, base : base + chan_n] = square[...]


def opening_kernel(breadth, noisy_ref, kernel_ref, start_ref, sums_ref, squares_ref, flat, taps):
    height, lat_n, _ = noisy_ref.shape
    token_n = height * breadth
    flat[...] = jnp.zeros(flat.shape, F32)
    for row in range(height):
        flat[0:lat_n, row * breadth : (row + 1) * breadth] = noisy_ref[row].astype(F32)
    taps[...] = jnp.zeros(taps.shape, F32)
    value = flat[...]
    lane = lax.broadcasted_iota(jnp.int32, value.shape, 1)
    column = lane % breadth
    for offset in range(9):
        row_off, col_off = offset // 3 - 1, offset % 3 - 1
        shift = -(row_off * breadth + col_off) % token_n
        moved = pltpu.roll(value, shift, 1) if shift else value
        good = (column + col_off >= 0) & (column + col_off < breadth)
        good = good & (lane + row_off * breadth >= 0) & (lane + row_off * breadth < token_n)
        moved = jnp.where(good, moved, 0.0)
        taps[offset * lat_n : (offset + 1) * lat_n, :] = moved[0:lat_n]
    block_n = min(512, token_n)
    for start in range(0, token_n, block_n):
        part = jnp.dot(
            kernel_ref[...],
            taps[:, start : start + block_n].astype(BF16),
            preferred_element_type=F32,
        ).astype(BF16)
        start_ref[:, start : start + block_n] = part
        wide = part.astype(F32)
        if start == 0:
            sums_ref[...] = lane_sums(wide)
            squares_ref[...] = lane_sums(wide * wide)
        else:
            sums_ref[...] += lane_sums(wide)
            squares_ref[...] += lane_sums(wide * wide)


def first_kernel(
    counts,
    rows,
    breadth,
    origin_ref,
    start_ref,
    sums_ref,
    squares_ref,
    gains_ref,
    wave_ref,
    bias_ref,
    *rest,
):
    pieces = rest[:counts]
    middle_ref, sums_out, squares_out = rest[counts : counts + 3]
    stage, weights, level, offset, mean, factor, hidden = rest[counts + 3 :]
    chan_n, token_n = start_ref.shape
    gains = gains_ref[...].T
    number = token_n * (chan_n // GROUPS)
    assemble(origin_ref, pieces, stage, rows, weights)
    conv_width = 9 * chan_n
    temb_n = hidden.shape[0]
    many = temb_n // chan_n
    for index in range(many):
        first = weights[:, conv_width + index * chan_n : conv_width + (index + 1) * chan_n]
        inner = jnp.dot(first, wave_ref[...], preferred_element_type=F32)
        for place in range(chan_n // rows):
            base = place * many * rows + index * rows
            hidden[base : base + rows, :] = inner[place * rows : (place + 1) * rows]
    second = weights[:, conv_width + temb_n : conv_width + 2 * temb_n]
    lifted = silu(silu(hidden[...] + bias_ref[...].T[:, 0:1])).astype(BF16)
    embedded = jnp.dot(second, lifted, preferred_element_type=F32)
    embedded = embedded[:, 0:1] + gains[:, 5:6]
    set_moments(
        sums_ref[...], squares_ref[...], number, gains[:, 0:1], EPS_BLOCK, mean, factor
    )
    normal_taps(start_ref, level, offset, mean, factor, breadth)
    block_n = min(512, token_n)
    for start in range(0, token_n, block_n):
        part = convolve(weights, level, offset, breadth, start, block_n)
        part = (part + embedded).astype(BF16)
        middle_ref[:, start : start + block_n] = part
        wide = part.astype(F32)
        if start == 0:
            sums_out[...] = lane_sums(wide)
            squares_out[...] = lane_sums(wide * wide)
        else:
            sums_out[...] += lane_sums(wide)
            squares_out[...] += lane_sums(wide * wide)


def second_kernel(
    counts,
    rows,
    breadth,
    origin_ref,
    space_ref,
    middle_ref,
    sums_ref,
    squares_ref,
    start_ref,
    gains_ref,
    *rest,
):
    pieces = rest[:counts]
    outputs = rest[counts : counts + 4]
    stage, weights, level, offset, mean, factor, sums, squares, block, tokens = rest[
        counts + 4 : counts + 14
    ]
    query_out, key_out, value_out = rest[counts + 14 : counts + 17]
    chan_n, token_n = middle_ref.shape
    gains = gains_ref[...].T
    query_n = query_out.shape[2]
    number = token_n * (chan_n // GROUPS)
    assemble(origin_ref, pieces, stage, rows, weights)
    conv_width = 9 * chan_n

    def small(index):
        base = conv_width + index * chan_n
        return weights[:, base : base + chan_n]

    set_moments(
        sums_ref[...], squares_ref[...], number, gains[:, 1:2], EPS_BLOCK, mean, factor
    )
    normal_taps(middle_ref, level, offset, mean, factor, breadth)
    block_n = min(512, token_n)
    for start in range(0, token_n, block_n):
        part = convolve(weights, level, offset, breadth, start, block_n)
        part = (part + start_ref[:, start : start + block_n].astype(F32)).astype(BF16)
        block[:, start : start + block_n] = part
        wide = part.astype(F32)
        if start == 0:
            sums[...] = lane_sums(wide)
            squares[...] = lane_sums(wide * wide)
        else:
            sums[...] += lane_sums(wide)
            squares[...] += lane_sums(wide * wide)
    set_moments(sums[...], squares[...], number, gains[:, 2:3], EPS_GROUP, mean, factor)
    own = pl.multiple_of(space_ref[0] * query_n, 128)

    def project(source):
        normed = ((source.astype(F32) - mean[:, 0:1]) * factor[:, 0:1]).astype(BF16)
        return jnp.dot(small(0), normed, preferred_element_type=F32)

    for start in range(0, token_n, block_n):
        projected = project(block[:, start : start + block_n])
        average = jnp.mean(projected, axis=0, keepdims=True)
        centred = projected - average
        spread = jnp.mean(centred * centred, axis=0, keepdims=True)
        scaled = centred * lax.rsqrt(spread + EPS_LAYER) * gains[:, 4:5]
        token = scaled.astype(BF16)
        tokens[:, start : start + block_n] = token
        value = jnp.dot(small(3), token, preferred_element_type=F32)
        ones = jnp.ones((8, block_n), F32)
        for head in range(HEADS):
            piece = value[head * HEAD_SIZE : (head + 1) * HEAD_SIZE]
            value_out[head, :, start : start + block_n] = jnp.concatenate(
                [piece, ones], axis=0
            ).astype(BF16)
        upright = token.T
        half = HEADS // 2 * HEAD_SIZE
        for part in range(2):
            matrix = weights[
                part * half : (part + 1) * half,
                conv_width + 2 * chan_n : conv_width + 3 * chan_n,
            ]
            key_out[part, start : start + block_n, :] = lax.dot_general(
                upright, matrix, (((1,), (1,)), ((), ())), preferred_element_type=F32
            ).astype(BF16)
    query = jnp.dot(small(1), tokens[:, pl.ds(own, query_n)], preferred_element_type=F32)
    query = query * (math.log2(math.e) / math.sqrt(HEAD_SIZE))
    per_half = HEADS // 2
    for head in range(HEADS):
        spot = head % per_half
        piece = query[head * HEAD_SIZE : (head + 1) * HEAD_SIZE]
        parts = []
        if spot:
            parts.append(jnp.zeros((spot * HEAD_SIZE, query_n), F32))
        parts.append(piece)
        if spot < per_half - 1:
            parts.append(jnp.zeros(((per_half - 1 - spot) * HEAD_SIZE, query_n), F32))
        query_out[head] = jnp.concatenate(parts, axis=0).astype(BF16)
    attend(query_out, key_out, value_out, *rest[counts + 17 :])
    attended = rest[counts + 17]
    mine = block[:, pl.ds(own, query_n)]
    mixture = jnp.dot(small(4), attended[...].astype(BF16), preferred_element_type=F32)
    mixture = (mixture + project(mine)).astype(BF16)
    outer = jnp.dot(small(5), mixture, preferred_element_type=F32)
    report((mine.astype(F32) + outer).astype(BF16), breadth, space_ref[0] == 0, *outputs)


def attend(query_ref, key_ref, value_ref, attended, *slots):
    heads, _, query_n = query_ref.shape
    token_n = key_ref.shape[1]
    width = slots[0].shape[1]
    blocks = query_n // width
    items = heads * blocks
    key_n = min(256, token_n)

    def spot(item):
        return item // blocks, pl.multiple_of((item % blocks) * width, 128)

    def step(item, scores, tops, ahead, scores_ahead, tops_ahead):
        head_ahead, base_ahead = spot(ahead)
        query = query_ref[head_ahead, :, pl.ds(base_ahead, width)]
        running = mixed = None
        if item is not None:
            head, base = spot(item)
            top = jnp.max(tops[...], axis=0, keepdims=True)
        for start in range(0, token_n, key_n):
            keys = key_ref[head_ahead // (heads // 2), start : start + key_n, :]
            part = jnp.dot(keys, query, preferred_element_type=F32)
            scores_ahead[start : start + key_n, :] = part
            part = jnp.max(part.reshape(key_n // 8, 8, width), axis=0)
            running = part if running is None else jnp.maximum(running, part)
            if item is not None:
                weight = jnp.exp2(scores[start : start + key_n, :] - top).astype(BF16)
                part = jnp.dot(
                    value_ref[head, :, start : start + key_n], weight, preferred_element_type=F32
                )
                mixed = part if mixed is None else mixed + part
        tops_ahead[...] = running
        if item is not None:
            row = pl.multiple_of(head * HEAD_SIZE, 8)
            attended[pl.ds(row, HEAD_SIZE), pl.ds(base, width)] = (
                mixed[:HEAD_SIZE] / mixed[HEAD_SIZE : HEAD_SIZE + 1]
            )

    even, odd = slots[0:2], slots[2:4]
    step(None, None, None, 0, *even)

    def two(index, carry):
        step(2 * index, *even, 2 * index + 1, *odd)
        step(2 * index + 1, *odd, jnp.minimum(2 * index + 2, items - 1), *even)
        return carry

    lax.fori_loop(0, items // 2, two, 0)


def report(block_two, breadth, first, block_two_ref, sums_ref, squares_ref, packed_ref):
    query_n = block_two.shape[1]
    block_two_ref[...] = block_two
    wide = block_two.astype(F32)
    sums = lane_sums(wide)
    squares = lane_sums(wide * wide)
    sums_ref[...] = sums
    squares_ref[...] = squares
    edge = jnp.where(first, wide[:, query_n - breadth :], wide[:, :breadth])
    packed_ref[...] = moment_columns(sums, squares, breadth).astype(BF16)
    packed_ref[:, :breadth] = edge.astype(BF16)


def closing_kernel(
    breadth,
    number,
    space_n,
    space_ref,
    weight_ref,
    block_ref,
    above_ref,
    below_ref,
    sums_ref,
    squares_ref,
    gains_ref,
    kernel_ref,
    noise_ref,
    out_ref,
    active,
):
    chan_n, token_n = block_ref.shape
    gains = gains_ref[...].T
    lat_n = noise_ref.shape[1]
    columns = moment_columns(sums_ref[...], squares_ref[...], 0)
    bases = (0,)
    if space_n == 2:
        lane = lax.broadcasted_iota(jnp.int32, columns.shape, 1)
        columns = jnp.where(lane >= breadth, above_ref[...].astype(F32), columns)
        bases = (0, breadth)
    mean, square = group_moments(columns, bases, number)
    factor = lax.rsqrt(square - mean * mean + EPS_BLOCK) * gains[:, 3:4]

    def act(value):
        return silu((value.astype(F32) - mean) * factor)

    first = space_ref[0] == 0
    last = space_ref[0] == space_n - 1
    margin = 2 * breadth
    top = jnp.where(first, 0.0, act(above_ref[:, :breadth]))
    end = jnp.where(last, 0.0, act(below_ref[:, :breadth]))
    blank = jnp.zeros((chan_n, breadth), F32)
    active[:, :margin] = jnp.concatenate([blank, top], axis=1).astype(BF16)
    active[:, margin : margin + token_n] = act(block_ref[...]).astype(BF16)
    active[:, margin + token_n :] = jnp.concatenate([end, blank], axis=1).astype(BF16)
    taps = jnp.dot(kernel_ref[...], active[...], preferred_element_type=F32)
    total_n = token_n + 2 * margin
    lane = lax.broadcasted_iota(jnp.int32, (8, token_n), 1)
    column = lane % breadth
    result = jnp.zeros((8, token_n), F32)
    for offset in range(9):
        row_off, col_off = offset // 3 - 1, offset % 3 - 1
        piece = taps[offset * 8 : (offset + 1) * 8]
        shift = -(row_off * breadth + col_off) % total_n
        moved = pltpu.roll(piece, shift, 1) if shift else piece
        moved = moved[:, margin : margin + token_n]
        good = (column + col_off >= 0) & (column + col_off < breadth)
        result = result + jnp.where(good, moved, 0.0)
    weight = weight_ref[0]
    for row in range(token_n // breadth):
        part = result[0:lat_n, row * breadth : (row + 1) * breadth]
        out_ref[row] = weight * (part - noise_ref[row])


def kernel_call(body, out_shape, scratch, scalars=0, flops=0):
    smem = pl.BlockSpec(memory_space=pltpu.SMEM)
    vmem = pl.BlockSpec(memory_space=pltpu.VMEM)
    cost = pl.CostEstimate(flops=flops, transcendentals=0, bytes_accessed=0) if flops else None

    def call(*args):
        return pl.pallas_call(
            body,
            out_shape=out_shape,
            in_specs=[smem] * scalars + [vmem] * (len(args) - scalars),
            scratch_shapes=scratch,
            compiler_params=pltpu.CompilerParams(vmem_limit_bytes=VMEM_BYTES),
            cost_estimate=cost,
        )(*args)

    return call


def body(
    latents,
    noise_draw,
    timesteps,
    inlet_conv,
    time_first,
    time_first_bias,
    time_second,
    time_second_bias,
    conv_first,
    conv_second,
    proj_inner,
    query_weight,
    key_weight,
    value_weight,
    attn_out,
    proj_outer,
    outlet_conv,
    first_gain,
    second_gain,
    third_gain,
    final_gain,
    layer_gain,
):
    shape = jax.ShapeDtypeStruct
    view_n, height, breadth, lat_n = latents.shape
    assert view_n == 1
    rows = conv_first.shape[1]
    chan_n = inlet_conv.shape[1]
    temb_n = time_first_bias.shape[0]
    space_n = lax.axis_size("space")
    place = lax.axis_index("space")
    token_n = height * space_n * breadth
    query_n = height * breadth

    squares = (proj_inner, query_weight, key_weight, value_weight, attn_out, proj_outer)
    shards = (conv_first, time_first, time_second, conv_second) + squares
    conv_width = conv_first.shape[0]
    width_one = conv_width + 2 * temb_n
    width_two = conv_width + len(squares) * chan_n
    batch_one, batch_two = kernel_call(
        pack_kernel,
        [shape((rows, width_one), BF16), shape((rows, width_two), BF16)],
        [],
    )(*(shard.T for shard in shards))

    moments = [shape((chan_n, 128), F32)] * 2
    taps_n = 9 * lat_n
    taps_pad = -(-taps_n // 16) * 16

    def early(steps):
        alpha_bar = lookup(steps)
        alpha_here = alpha_bar[:, None, None, None]
        noisy = jnp.sqrt(alpha_here) * latents + jnp.sqrt(1.0 - alpha_here) * noise_draw
        noisy = noisy.astype(BF16)[0].transpose(0, 2, 1)
        if space_n == 2:
            other = lax.ppermute(noisy, "space", [(0, 1), (1, 0)])
            noisy = jnp.stack([noisy, other])
            noisy = jnp.where(place == 0, noisy, noisy[::-1]).reshape(2 * height, lat_n, breadth)
        else:
            noisy = lax.all_gather(noisy, "space", axis=0, tiled=True)
        inlet = jnp.pad(inlet_conv.T, ((0, 0), (0, taps_pad - taps_n)))
        opened = kernel_call(
            lambda *refs: opening_kernel(breadth, *refs),
            [shape((chan_n, token_n), BF16)] + moments,
            [pltpu.VMEM((8, token_n), F32), pltpu.VMEM((taps_pad, token_n), F32)],
        )(noisy, inlet)
        return opened, alpha_bar

    def later(steps):
        wave = waveform_of(steps, chan_n // 2)
        wave = jnp.broadcast_to(wave.reshape(chan_n, 1), (chan_n, 128))
        gains = (first_gain, second_gain, third_gain, final_gain, layer_gain, time_second_bias)
        gains = jnp.stack(gains + (layer_gain,) * 2)
        outlet = outlet_conv.T.reshape(lat_n, 9, chan_n).transpose(1, 0, 2)
        outlet = jnp.pad(outlet, ((0, 0), (0, 8 - lat_n), (0, 0))).reshape(72, chan_n)
        bias = jnp.broadcast_to(time_first_bias[None], (8, temb_n))
        return wave, gains, outlet, bias

    (pieces_one, pieces_two), origin, extra = gather_shards(
        batch_one, batch_two, timesteps, (early, later)
    )
    ((start, sums, squares), alpha_bar), (wave, gains, outlet, bias) = extra
    space_id = place.reshape(1).astype(jnp.int32)

    count_one = len(pieces_one)
    deep = sum(padded(piece.shape[0]) for piece in pieces_one)
    deep_two = sum(padded(piece.shape[0]) for piece in pieces_two)
    args = (origin, start, sums, squares, gains, wave, bias, *pieces_one)
    middle, sums, squares = kernel_call(
        lambda *refs: first_kernel(count_one, rows, breadth, *refs),
        [shape((chan_n, token_n), BF16)] + moments,
        [
            pltpu.VMEM((deep, width_one), BF16),
            pltpu.VMEM((chan_n, width_one), BF16),
            pltpu.VMEM((3 * chan_n, token_n), BF16),
            pltpu.VMEM((3 * chan_n, token_n + 2 * breadth), BF16),
            pltpu.VMEM((chan_n, 128), F32),
            pltpu.VMEM((chan_n, 128), F32),
            pltpu.VMEM((temb_n, 128), F32),
        ],
        1,
        2 * token_n * conv_width * chan_n,
    )(*args)

    count_two = len(pieces_two)
    half = HEADS // 2 * HEAD_SIZE
    args = (origin, space_id, middle, sums, squares, start, gains, *pieces_two)
    width = min(512, query_n)
    block_two, sums, squares, packed = kernel_call(
        lambda *refs: second_kernel(count_two, rows, breadth, *refs),
        [shape((chan_n, query_n), BF16)] + moments + [shape((chan_n, 128), BF16)],
        [
            pltpu.VMEM((deep_two, width_two), BF16),
            pltpu.VMEM((chan_n, width_two), BF16),
            pltpu.VMEM((3 * chan_n, token_n), BF16),
            pltpu.VMEM((3 * chan_n, token_n + 2 * breadth), BF16),
            pltpu.VMEM((chan_n, 128), F32),
            pltpu.VMEM((chan_n, 128), F32),
            pltpu.VMEM((chan_n, 128), F32),
            pltpu.VMEM((chan_n, 128), F32),
            pltpu.VMEM((chan_n, token_n), BF16),
            pltpu.VMEM((chan_n, token_n), BF16),
            pltpu.VMEM((HEADS, half, query_n), BF16),
            pltpu.VMEM((2, token_n, half), BF16),
            pltpu.VMEM((HEADS, HEAD_SIZE + 8, token_n), BF16),
            pltpu.VMEM((chan_n, query_n), F32),
        ]
        + [pltpu.VMEM((token_n, width), F32), pltpu.VMEM((8, width), F32)] * 2,
        2,
    )(*args)

    if space_n == 2:
        above = below = lax.ppermute(packed, "space", [(0, 1), (1, 0)])
    else:
        sums, squares = lax.psum((sums, squares), "space")
        ahead = [(i, i + 1) for i in range(space_n - 1)]
        above = lax.ppermute(block_two[:, query_n - breadth :], "space", ahead)
        below = lax.ppermute(block_two[:, :breadth], "space", [(j, i) for i, j in ahead])
    number = token_n * (chan_n // GROUPS)
    args = (
        space_id,
        1.0 - alpha_bar,
        block_two,
        above,
        below,
        sums,
        squares,
        gains,
        outlet,
        noise_draw[0].transpose(0, 2, 1),
    )
    out = kernel_call(
        lambda *refs: closing_kernel(breadth, number, space_n, *refs),
        shape((height, lat_n, breadth), F32),
        [pltpu.VMEM((chan_n, query_n + 4 * breadth), BF16)],
        2,
    )(*args)
    return out.transpose(0, 2, 1)[None]


def solution(mesh):
    split = P(None, "batch")
    view = P("batch", "space", None, None)
    in_specs = (view, view, P("batch"), P(), split, P(), split, P())
    in_specs = in_specs + (split,) * 8 + (P(),) * 6

    return jax.shard_map(body, mesh=mesh, in_specs=in_specs, out_specs=view, check_vma=False)
```
